16 devices in a mesh: dp: 4 (over z, y), fsdp: 4 (over x, core).
Axes of the slice: x: 2, y: 2, z: 2, core: 2. Of those that a mesh axis runs over, the one named last changes fastest.
Arguments:
- u_in: bfloat16 [16, 1024, 1024], P(('dp', 'fsdp'))
- grad_out: bfloat16 [16, 1024, 1024], P(('dp', 'fsdp'))
- norm_w: bfloat16 [2, 1024], P(None, 'fsdp')
- w_in: bfloat16 [2, 1024, 4384], P(None, 'fsdp')
- conv_w: bfloat16 [2, 4, 2304], P(None, None, 'fsdp')
- conv_b: bfloat16 [2, 2304], P(None, 'fsdp')
- dt_bias: float32 [2, 32], P(None, 'fsdp')
- a_log: float32 [2, 32], P(None, 'fsdp')
- d_skip: float32 [2, 32], P(None, 'fsdp')
- gate_w: bfloat16 [2, 2048], P(None, 'fsdp')
- w_out: bfloat16 [2, 2048, 1024], P(None, 'fsdp')
Outputs:
- output 1: bfloat16 [16, 1024, 1024], P(('dp', 'fsdp'))
- output 2: bfloat16 [16, 1024, 1024], P(('dp', 'fsdp'))
- output 3: float32 [2, 1024], P(None, 'fsdp')
- output 4: float32 [2, 1024, 4384], P(None, 'fsdp')
- output 5: float32 [2, 4, 2304], P(None, None, 'fsdp')
- output 6: float32 [2, 2304], P(None, 'fsdp')
- output 7: float32 [2, 32], P(None, 'fsdp')
- output 8: float32 [2, 32], P(None, 'fsdp')
- output 9: float32 [2, 32], P(None, 'fsdp')
- output 10: float32 [2, 2048], P(None, 'fsdp')
- output 11: float32 [2, 2048, 1024], P(None, 'fsdp')
All inputs are finite; a program needn't handle non-finite values.
Results may differ from the reference program's by a relative error of at most 0.02.
Values are sent between devices in bfloat16 or wider.
A program may use at most 1 GiB of HBM per device.

```python
import jax
import jax.numpy as jnp
from jax import lax

D_MODEL = 1024
D_INNER = 2048
N_HEADS = 32
HEAD_DIM = 64
D_STATE = 128
N_GROUPS = 1
CONV_WIDTH = 4
CHUNK_LEN = 256
SEQ_LEN = 1024
BATCH_TOT = 16
CONV_DIM = D_INNER + 2 * N_GROUPS * D_STATE
PROJ_DIM = 2 * D_INNER + 2 * N_GROUPS * D_STATE + N_HEADS
PER_GROUP = N_HEADS // N_GROUPS
NORM_EPS = 1e-5


def setup_inputs(seed: int = 0) -> dict:
    keys = jax.random.split(jax.random.key(seed), 11)

    def normal(key_i, shape, scale):
        return jax.random.normal(key_i, shape, jnp.float32) * scale

    act_shape = (BATCH_TOT, SEQ_LEN, D_MODEL)
    return {
        'u_in': normal(keys[0], act_shape, 1.0).astype(jnp.bfloat16),
        'grad_out': normal(keys[1], act_shape, 1.0).astype(jnp.bfloat16),
        'norm_w': (1.0 + normal(keys[2], (2, D_MODEL), 0.3)).astype(jnp.bfloat16),
        'w_in': normal(keys[3], (2, D_MODEL, PROJ_DIM), D_MODEL ** -0.5).astype(jnp.bfloat16),
        'conv_w': normal(keys[4], (2, CONV_WIDTH, CONV_DIM), CONV_WIDTH ** -0.5).astype(jnp.bfloat16),
        'conv_b': normal(keys[5], (2, CONV_DIM), 0.5).astype(jnp.bfloat16),
        'dt_bias': normal(keys[6], (2, N_HEADS), 1.0) - 2.0,
        'a_log': jnp.log(jax.random.uniform(keys[7], (2, N_HEADS), jnp.float32, 1.0, 16.0)),
        'd_skip': 1.0 + normal(keys[8], (2, N_HEADS), 0.5),
        'gate_w': (1.0 + normal(keys[9], (2, D_INNER), 0.3)).astype(jnp.bfloat16),
        'w_out': normal(keys[10], (2, D_INNER, D_MODEL), D_INNER ** -0.5).astype(jnp.bfloat16),
    }


def pre_norm(u_rows, norm_w):
    rows_f = u_rows.astype(jnp.float32)
    inv_rms = lax.rsqrt(jnp.mean(rows_f * rows_f, axis=-1, keepdims=True) + NORM_EPS)
    return (rows_f * inv_rms * norm_w.astype(jnp.float32)).astype(jnp.bfloat16)


def ssd_chunks(x_heads, dt_heads, a_heads, b_mat, c_mat):
    n_chunks = x_heads.shape[0] // CHUNK_LEN
    x_dt = (x_heads * dt_heads[:, :, None]).reshape(n_chunks, CHUNK_LEN, N_GROUPS, PER_GROUP, HEAD_DIM)
    cum_a = jnp.cumsum(a_heads.reshape(n_chunks, CHUNK_LEN, N_GROUPS, PER_GROUP), axis=1)
    b_chunk = b_mat.reshape(n_chunks, CHUNK_LEN, N_GROUPS, D_STATE).astype(jnp.float32)
    c_chunk = c_mat.reshape(n_chunks, CHUNK_LEN, N_GROUPS, D_STATE).astype(jnp.float32)
    scores = jnp.einsum('cqgn,csgn->cgqs', c_chunk, b_chunk)
    cum_t = jnp.moveaxis(cum_a, 1, -1)
    log_gap = cum_t[..., :, None] - cum_t[..., None, :]
    causal = jnp.arange(CHUNK_LEN)[:, None] >= jnp.arange(CHUNK_LEN)[None, :]
    decay_mat = jnp.where(causal, jnp.exp(jnp.where(causal, log_gap, 0.0)), 0.0)
    y_diag = jnp.einsum('cgrqs,csgrp->cqgrp', scores[:, :, None] * decay_mat, x_dt)
    end_decay = jnp.exp(cum_a[:, -1:] - cum_a)
    states = jnp.einsum('csgn,csgrp->cgrpn', b_chunk, x_dt * end_decay[..., None])
    totals = cum_a[:, -1]
    incl_sum = jnp.cumsum(totals, axis=0)
    excl_sum = incl_sum - totals
    chunk_gap = jnp.moveaxis(excl_sum, 0, -1)[..., :, None] - jnp.moveaxis(incl_sum, 0, -1)[..., None, :]
    earlier = jnp.arange(n_chunks)[:, None] > jnp.arange(n_chunks)[None, :]
    carry_mat = jnp.where(earlier, jnp.exp(jnp.where(earlier, chunk_gap, 0.0)), 0.0)
    prev_state = jnp.einsum('grij,jgrpn->igrpn', carry_mat, states)
    y_off = jnp.einsum('cqgn,cgrpn->cqgrp', c_chunk, prev_state) * jnp.exp(cum_a)[..., None]
    return (y_diag + y_off).reshape(x_heads.shape)


def mamba_layer(u_seq, layer_w):
    norm_w, w_in, conv_w, conv_b, dt_bias, a_log, d_skip, gate_w, w_out = layer_w
    seq_len = u_seq.shape[0]
    h_norm = pre_norm(u_seq, norm_w)
    proj_out = jnp.dot(h_norm, w_in, preferred_element_type=jnp.float32).astype(jnp.bfloat16)
    xbc = proj_out[:, D_INNER:D_INNER + CONV_DIM].astype(jnp.float32)
    padded = jnp.pad(xbc, ((CONV_WIDTH - 1, 0), (0, 0)))
    conv_out = conv_b.astype(jnp.float32) + sum(padded[tap:tap + seq_len] * conv_w[tap].astype(jnp.float32) for tap in range(CONV_WIDTH))
    xbc_act = jax.nn.silu(conv_out)
    group_w = N_GROUPS * D_STATE
    x_heads = xbc_act[:, :D_INNER].reshape(seq_len, N_HEADS, HEAD_DIM)
    b_mat = xbc_act[:, D_INNER:D_INNER + group_w].reshape(seq_len, N_GROUPS, D_STATE)
    c_mat = xbc_act[:, D_INNER + group_w:].reshape(seq_len, N_GROUPS, D_STATE)
    dt_heads = jax.nn.softplus(proj_out[:, D_INNER + CONV_DIM:].astype(jnp.float32) + dt_bias)
    a_heads = dt_heads * -jnp.exp(a_log)
    y_heads = ssd_chunks(x_heads, dt_heads, a_heads, b_mat, c_mat) + d_skip[:, None] * x_heads
    z_act = jax.nn.silu(proj_out[:, :D_INNER].astype(jnp.float32))
    gated_y = y_heads.reshape(seq_len, N_GROUPS, -1) * z_act.reshape(seq_len, N_GROUPS, -1)
    normed = gated_y * lax.rsqrt(jnp.mean(gated_y * gated_y, axis=-1, keepdims=True) + NORM_EPS)
    y_norm = (normed.reshape(seq_len, D_INNER) * gate_w.astype(jnp.float32)).astype(jnp.bfloat16)
    mixed = jnp.dot(y_norm, w_out, preferred_element_type=jnp.float32)
    return (u_seq.astype(jnp.float32) + mixed).astype(jnp.bfloat16)


def reference(u_in, grad_out, norm_w, w_in, conv_w, conv_b, dt_bias, a_log, d_skip, gate_w, w_out):
    params = (norm_w, w_in, conv_w, conv_b, dt_bias, a_log, d_skip, gate_w, w_out)

    def two_layers(u_seq, stack_w):
        hidden = mamba_layer(u_seq, [w_l[0] for w_l in stack_w])
        return mamba_layer(hidden, [w_l[1] for w_l in stack_w])

    def per_sequence(acc, pair):
        u_seq, g_seq = pair
        out_seq, pull = jax.vjp(two_layers, u_seq, params)
        du_seq, d_params = pull(g_seq)
        acc = tuple(total + grad_w.astype(jnp.float32) for total, grad_w in zip(acc, d_params))
        return acc, (out_seq, du_seq)

    zeros = tuple(jnp.zeros(w_l.shape, jnp.float32) for w_l in params)
    sums, (out, d_u) = lax.scan(per_sequence, zeros, (u_in, grad_out))
    return (out, d_u) + tuple(total / BATCH_TOT for total in sums)
```

```python
import functools
import jax
import jax.numpy as jnp
from jax import lax
from jax.sharding import PartitionSpec as P
from jax.experimental import pallas as pl
from jax.experimental.pallas import tpu as pltpu

F32 = jnp.float32
BF16 = jnp.bfloat16
NORM_EPS = 1e-5
LOG2E = 1.4426950408889634
Q = 128
HP = 64
NS = 128
NN = (((1,), (0,)), ((), ()))
NT = (((1,), (1,)), ((), ()))
TN = (((0,), (0,)), ((), ()))


def mm(a, b, dims=NN):
    return lax.dot_general(a, b, dims, preferred_element_type=F32)


def sigm(v):
    return 0.5 * jnp.tanh(0.5 * v) + 0.5


def lane_iota(rows):
    return lax.broadcasted_iota(jnp.int32, (rows, Q), 1)


def ssd_fwd_kernel(n_heads, pz_ref, px_ref, pdt_ref, cw_ref, gw_ref, hv_ref,
                   n_ref, y_ref, s_ref, cv_ref, r_ref, dt_ref, cum_ref, cumt_ref,
                   wb, gb, xprev, xs, vs, gt_s, st, rows_s):
    step = pl.program_id(0)
    d_inner = n_heads * HP
    conv_dim = d_inner + 2 * NS
    seq = dt_ref.shape[1]
    n_chunk = seq // Q

    @pl.when(step == 0)
    def _():
        @pl.loop(0, conv_dim // 64)
        def _(i):
            rr = pl.ds(pl.multiple_of(i * 64, 64), 64)
            for k in range(5):
                wb[k, rr, :] = jnp.broadcast_to(cw_ref[rr, k:k + 1], (64, Q))
            xprev[rr, :] = jnp.zeros((64, Q), BF16)

        @pl.loop(0, d_inner // 64)
        def _(i):
            rr = pl.ds(pl.multiple_of(i * 64, 64), 64)
            gb[rr, :] = jnp.broadcast_to(gw_ref[rr, 0:1], (64, Q))
            st[rr, :] = jnp.zeros((64, NS), F32)
        lane = lane_iota(n_heads)
        for c in range(n_chunk):
            cc = slice(c * Q, (c + 1) * Q)
            raw = pdt_ref[:, cc].astype(F32) + hv_ref[0]
            dt = jnp.maximum(raw, 0.0) + jnp.log1p(jnp.exp(-jnp.abs(raw)))
            acc = dt * hv_ref[1]
            for k in (1, 2, 4, 8, 16, 32, 64):
                acc = acc + jnp.where(lane >= k, pltpu.roll(acc, k, 1), 0.0)
            dt_ref[:, cc] = dt
            cum_ref[:, cc] = acc
            cumt_ref[cc, :] = jnp.transpose(acc)

    cs = pl.ds(pl.multiple_of(step * Q, Q), Q)

    @pl.loop(0, conv_dim // 64)
    def _(i):
        rr = pl.ds(pl.multiple_of(i * 64, 64), 64)
        lane = lane_iota(64)
        raw = px_ref[rr, :]
        x = raw.astype(F32)
        xp = xprev[rr, :].astype(F32)
        xprev[rr, :] = raw
        acc = wb[4, rr, :] + wb[3, rr, :] * x
        for j in (1, 2, 3):
            sh = pltpu.roll(jnp.where(lane >= Q - j, xp, x), j, 1)
            acc = acc + wb[3 - j, rr, :] * sh
        cv_ref[rr, :] = acc
        xs[rr, :] = acc * sigm(acc)

    bt = xs[d_inner:d_inner + NS, :].astype(BF16)
    ct = xs[d_inner + NS:, :].astype(BF16)
    causal = lax.broadcasted_iota(jnp.int32, (Q, Q), 0) <= lax.broadcasted_iota(jnp.int32, (Q, Q), 1)
    gt_s[...] = jnp.where(causal, mm(bt, ct, TN), 0.0)
    cum = cum_ref[:, cs]
    tot = jnp.broadcast_to(cum[:, Q - 1:Q], (n_heads, Q))
    rows_s[0] = jnp.exp(cum)
    rows_s[1] = jnp.exp(tot - cum)
    rows_s[2] = jnp.exp(tot)
    rows_s[3] = cum * LOG2E
    rows_s[4] = dt_ref[:, cs]
    rows_s[5] = hv_ref[2]
    cumt = cumt_ref[cs, :] * LOG2E

    grp = 4
    ssq = jnp.zeros((8, Q), F32)
    for g in range(n_heads // grp):
        gg = slice(g * grp * HP, (g + 1) * grp * HP)
        st_g = st[gg, :]
        s_ref[0, gg, :] = st_g
        yoff = mm(st_g.astype(BF16), ct)
        xe = []
        for k in range(grp):
            h = g * grp + k
            hh = slice(h * HP, (h + 1) * HP)
            x = xs[hh, :]
            xdt = x * rows_s[4, h:h + 1, :]
            gap = rows_s[3, h:h + 1, :] - cumt[:, h:h + 1]
            mt = (gt_s[...] * jnp.exp2(jnp.minimum(gap, 0.0))).astype(BF16)
            y = mm(xdt.astype(BF16), mt) + yoff[k * HP:(k + 1) * HP, :] * rows_s[0, h:h + 1, :]
            y_ref[hh, :] = y
            z = pz_ref[hh, :].astype(F32)
            v = (y + rows_s[5, h:h + 1, :] * x) * (z * sigm(z))
            vs[hh, :] = v
            sq = v * v
            for b in range(HP // 8):
                ssq = ssq + sq[b * 8:(b + 1) * 8, :]
            xe.append((xdt * rows_s[1, h:h + 1, :]).astype(BF16))
        upd = mm(jnp.concatenate(xe, axis=0), bt, NT)
        for k in range(grp):
            h = g * grp + k
            hh = slice(h * HP, (h + 1) * HP)
            st[hh, :] = st[hh, :] * rows_s[2, h:h + 1, :] + upd[k * HP:(k + 1) * HP, :]

    r = lax.rsqrt(jnp.sum(ssq, axis=0, keepdims=True) / d_inner + NORM_EPS)
    r_ref[:, :] = r

    @pl.loop(0, d_inner // 128)
    def _(i):
        rr = pl.ds(pl.multiple_of(i * 128, 128), 128)
        n_ref[rr, :] = (vs[rr, :] * r * gb[rr, :]).astype(BF16)


def ssd_fwd(pz, px, conv_w, conv_b, dt_bias, a_log, d_skip, gate_w):
    d_inner, seq = pz.shape
    conv_dim = conv_b.shape[0]
    n_heads = dt_bias.shape[0]
    n_chunk = seq // Q
    cw = jnp.concatenate([conv_w.astype(F32), conv_b.astype(F32)[None]], axis=0).T
    gw = gate_w.astype(F32)[:, None]
    hv = jnp.broadcast_to(jnp.stack([dt_bias, -jnp.exp(a_log), d_skip])[:, :, None], (3, n_heads, Q))
    pdt = px[conv_dim:]
    full = lambda s: pl.BlockSpec(s, lambda c: (0,) * len(s))
    tok = lambda rows: pl.BlockSpec((rows, Q), lambda c: (0, c))
    return pl.pallas_call(
        functools.partial(ssd_fwd_kernel, n_heads),
        grid=(n_chunk,),
        in_specs=[tok(d_inner), tok(conv_dim + n_heads), full((n_heads, seq)), full(cw.shape), full(gw.shape), full(hv.shape)],
        out_specs=[tok(d_inner), tok(d_inner), pl.BlockSpec((1, d_inner, NS), lambda c: (c, 0, 0)), tok(conv_dim), tok(1),
                   full((n_heads, seq)), full((n_heads, seq)), full((seq, n_heads))],
        out_shape=[jax.ShapeDtypeStruct((d_inner, seq), BF16), jax.ShapeDtypeStruct((d_inner, seq), F32),
                   jax.ShapeDtypeStruct((n_chunk, d_inner, NS), F32), jax.ShapeDtypeStruct((conv_dim, seq), F32),
                   jax.ShapeDtypeStruct((1, seq), F32), jax.ShapeDtypeStruct((n_heads, seq), F32),
                   jax.ShapeDtypeStruct((n_heads, seq), F32), jax.ShapeDtypeStruct((seq, n_heads), F32)],
        scratch_shapes=[pltpu.VMEM((5, conv_dim, Q), F32), pltpu.VMEM((d_inner, Q), F32), pltpu.VMEM((conv_dim, Q), BF16),
                        pltpu.VMEM((conv_dim, Q), F32), pltpu.VMEM((d_inner, Q), F32), pltpu.VMEM((Q, Q), F32),
                        pltpu.VMEM((d_inner, NS), F32), pltpu.VMEM((6, n_heads, Q), F32)],
        compiler_params=pltpu.CompilerParams(dimension_semantics=("arbitrary",), vmem_limit_bytes=56 << 20),
        cost_estimate=pl.CostEstimate(flops=30_000_000_000, bytes_accessed=40_000_000, transcendentals=0),
        name="ssd_fwd",
    )(pz, px, pdt, cw, gw, hv)


def gate_bwd_kernel(n_heads, pz_ref, y_ref, cv_ref, dn_ref, r_ref, gw_ref, hv_ref,
                    dz_ref, dy_ref, gg_ref, gb, sk):
    step = pl.program_id(0)
    d_inner = n_heads * HP

    @pl.when(step == 0)
    def _():
        @pl.loop(0, n_heads)
        def _(i):
            rr = pl.ds(pl.multiple_of(i * HP, HP), HP)
            gb[rr, :] = jnp.broadcast_to(gw_ref[rr, 0:1], (HP, Q))
            gg_ref[rr, :] = jnp.zeros((HP, Q), F32)
        sk[...] = hv_ref[2]
    r = r_ref[:, :]

    def yfull(i, rr):
        cv = cv_ref[rr, :]
        return y_ref[rr, :] + sk[pl.ds(i, 1), :] * (cv * sigm(cv))

    def pass1(i, acc):
        rr = pl.ds(pl.multiple_of(i * HP, HP), HP)
        z = pz_ref[rr, :].astype(F32)
        yf = yfull(i, rr)
        dy_ref[rr, :] = yf
        nrm = yf * (z * sigm(z)) * r
        t = dn_ref[rr, :].astype(F32) * nrm
        gg_ref[rr, :] = gg_ref[rr, :] + t
        t = t * gb[rr, :]
        for b in range(HP // 8):
            acc = acc + t[b * 8:(b + 1) * 8, :]
        return acc
    acc = lax.fori_loop(0, n_heads, pass1, jnp.zeros((8, Q), F32))
    mean = jnp.sum(acc, axis=0, keepdims=True) / d_inner

    @pl.loop(0, n_heads)
    def _(i):
        rr = pl.ds(pl.multiple_of(i * HP, HP), HP)
        z = pz_ref[rr, :].astype(F32)
        yf = dy_ref[rr, :]
        sg = sigm(z)
        sl = z * sg
        dv = r * (dn_ref[rr, :].astype(F32) * gb[rr, :] - (yf * sl * r) * mean)
        dy_ref[rr, :] = dv * sl
        dz_ref[rr, :] = (dv * yf * (sg + sl * (1.0 - sg))).astype(BF16)


def gate_bwd(pz, y, cv, dn, r, gate_w, d_skip):
    d_inner, seq = pz.shape
    n_heads = d_skip.shape[0]
    n_chunk = seq // Q
    gw = gate_w.astype(F32)[:, None]
    hv = jnp.broadcast_to(jnp.stack([d_skip, d_skip, d_skip])[:, :, None], (3, n_heads, Q))
    full = lambda s: pl.BlockSpec(s, lambda c: (0,) * len(s))
    tok = lambda rows: pl.BlockSpec((rows, Q), lambda c: (0, c))
    return pl.pallas_call(
        functools.partial(gate_bwd_kernel, n_heads),
        grid=(n_chunk,),
        in_specs=[tok(d_inner), tok(d_inner), tok(d_inner), tok(d_inner), tok(1), full(gw.shape), full(hv.shape)],
        out_specs=[tok(d_inner), tok(d_inner), full((d_inner, Q))],
        out_shape=[jax.ShapeDtypeStruct((d_inner, seq), BF16), jax.ShapeDtypeStruct((d_inner, seq), F32),
                   jax.ShapeDtypeStruct((d_inner, Q), F32)],
        scratch_shapes=[pltpu.VMEM((d_inner, Q), F32), pltpu.VMEM((n_heads, Q), F32)],
        compiler_params=pltpu.CompilerParams(dimension_semantics=("arbitrary",), vmem_limit_bytes=56 << 20),
        cost_estimate=pl.CostEstimate(flops=15_000_000_000, bytes_accessed=40_000_000, transcendentals=0),
        name="gate_bwd",
    )(pz, y, cv, dn, r, gw, hv)


def ssd_bwd_kernel(n_heads, n_chunk, px_ref, cv_ref, y_ref, dy_ref, s_ref, dt_ref, cum_ref, cumt_ref, cw_ref, hv_ref,
                   dpx_ref, gcw_ref, gh_ref,
                   wb, acc_w, dnext, ds, gt_s, dg_s, rows_s, red_s, dbc):
    step = pl.program_id(0)
    d_inner = n_heads * HP
    conv_dim = d_inner + 2 * NS

    @pl.when(step == 0)
    def _():
        @pl.loop(0, conv_dim // 64)
        def _(i):
            rr = pl.ds(pl.multiple_of(i * 64, 64), 64)
            for k in range(5):
                wb[k, rr, :] = jnp.broadcast_to(cw_ref[rr, k:k + 1], (64, Q))
                acc_w[k, rr, :] = jnp.zeros((64, Q), F32)
            dnext[rr, :] = jnp.zeros((64, Q), F32)

        @pl.loop(0, n_heads)
        def _(i):
            ds[pl.ds(pl.multiple_of(i * HP, HP), HP), :] = jnp.zeros((HP, NS), F32)
        gh_ref[...] = jnp.zeros(gh_ref.shape, F32)

    def conv_bwd(rr, dcv):
        n_rows = dcv.shape[0]
        lane = lane_iota(n_rows)
        raw = px_ref[rr, :].astype(F32)
        nxt = dnext[rr, :]
        dnext[rr, :] = dcv
        acc_w[4, rr, :] = acc_w[4, rr, :] + dcv
        acc_w[3, rr, :] = acc_w[3, rr, :] + dcv * raw
        dx = wb[3, rr, :] * dcv
        for j in (1, 2, 3):
            sh = pltpu.roll(jnp.where(lane < j, nxt, dcv), Q - j, 1)
            acc_w[3 - j, rr, :] = acc_w[3 - j, rr, :] + sh * raw
            dx = dx + wb[3 - j, rr, :] * sh
        dpx_ref[rr, :] = dx.astype(BF16)

    def act(cv):
        sg = sigm(cv)
        a = cv * sg
        return a, sg + a * (1.0 - sg)

    br = slice(d_inner, d_inner + NS)
    cr = slice(d_inner + NS, conv_dim)
    b_act, b_der = act(cv_ref[br, :])
    c_act, c_der = act(cv_ref[cr, :])
    bt = b_act.astype(BF16)
    ct = c_act.astype(BF16)
    causal = lax.broadcasted_iota(jnp.int32, (Q, Q), 0) <= lax.broadcasted_iota(jnp.int32, (Q, Q), 1)
    gt_s[...] = jnp.where(causal, mm(bt, ct, TN), 0.0)
    dg_s[...] = jnp.zeros((Q, Q), F32)
    cum = cum_ref[...]
    tot = jnp.broadcast_to(cum[:, Q - 1:Q], (n_heads, Q))
    rows_s[0] = jnp.exp(cum)
    rows_s[1] = jnp.exp(tot - cum)
    rows_s[2] = jnp.exp(tot)
    rows_s[3] = cum * LOG2E
    rows_s[4] = dt_ref[...]
    rows_s[5] = hv_ref[2]
    cumt = cumt_ref[...] * LOG2E
    dbc[...] = jnp.zeros(dbc.shape, F32)

    grp = 4
    for g in range(n_heads // grp):
        gg = slice(g * grp * HP, (g + 1) * grp * HP)
        ds_b = ds[gg, :].astype(BF16)
        sp_b = s_ref[0, gg, :].astype(BF16)
        dsb = mm(ds_b, bt)
        dye = []
        xde = []
        for k in range(grp):
            h = g * grp + k
            hh = slice(h * HP, (h + 1) * HP)
            kk = slice(k * HP, (k + 1) * HP)
            row = lambda a: rows_s[a, h:h + 1, :]
            x, der = act(cv_ref[hh, :])
            xdt = x * row(4)
            xdt_b = xdt.astype(BF16)
            dy = dy_ref[hh, :]
            dy_b = dy.astype(BF16)
            dmt = mm(xdt_b, dy_b, TN)
            dec = jnp.exp2(jnp.minimum(row(3) - cumt[:, h:h + 1], 0.0))
            mt = (gt_s[...] * dec).astype(BF16)
            dg_s[...] = dg_s[...] + dmt * dec
            t2 = dsb[kk, :] * row(1)
            dxdt = mm(dy_b, mt, NT) + t2
            dx = dxdt * row(4) + row(5) * dy
            xdt_r = xdt_b.astype(F32)
            red_s[0, h:h + 1, :] = jnp.sum(dxdt * x, axis=0, keepdims=True)
            red_s[1, h:h + 1, :] = jnp.sum(dy_b.astype(F32) * y_ref[hh, :] - xdt_r * dxdt, axis=0, keepdims=True)
            w_row = jnp.sum(ds[hh, :] * s_ref[0, hh, :], axis=0, keepdims=True)
            red_s[2, h:h + 1, :] = jnp.sum(xdt_r * t2, axis=0, keepdims=True) + row(2) * w_row
            gh_ref[2, h:h + 1, :] = gh_ref[2, h:h + 1, :] + jnp.sum(dy * x, axis=0, keepdims=True)
            dye.append((dy * row(0)).astype(BF16))
            xde.append((xdt * row(1)).astype(BF16))
            conv_bwd(hh, dx * der)
        dye = jnp.concatenate(dye, axis=0)
        xde = jnp.concatenate(xde, axis=0)
        dbc[0] = dbc[0] + mm(ds_b, xde, TN)
        dbc[1] = dbc[1] + mm(sp_b, dye, TN)
        upd = mm(dye, ct, NT)
        for k in range(grp):
            h = g * grp + k
            hh = slice(h * HP, (h + 1) * HP)
            ds[hh, :] = ds[hh, :] * rows_s[2, h:h + 1, :] + upd[k * HP:(k + 1) * HP, :]

    dg = jnp.where(causal, dg_s[...], 0.0).astype(BF16)
    conv_bwd(br, (dbc[0] + mm(ct, dg, NT)) * b_der)
    conv_bwd(cr, (dbc[1] + mm(bt, dg)) * c_der)

    lane = lane_iota(n_heads)
    suf = red_s[1]
    for k in (1, 2, 4, 8, 16, 32, 64):
        suf = suf + jnp.where(lane < Q - k, pltpu.roll(suf, Q - k, 1), 0.0)
    d_a = suf + jnp.broadcast_to(jnp.sum(red_s[2], axis=1, keepdims=True), (n_heads, Q))
    dt = dt_ref[...]
    raw = px_ref[conv_dim:, :].astype(F32) + hv_ref[0]
    d_raw = (red_s[0] + d_a * hv_ref[1]) * sigm(raw)
    dpx_ref[conv_dim:, :] = d_raw.astype(BF16)
    gh_ref[0] = gh_ref[0] + d_raw
    gh_ref[1] = gh_ref[1] + d_a * dt * hv_ref[1]

    @pl.when(step == n_chunk - 1)
    def _():
        @pl.loop(0, conv_dim // 64)
        def _(i):
            rr = pl.ds(pl.multiple_of(i * 64, 64), 64)
            lane = lane_iota(64)
            out = jnp.zeros((64, Q), F32)
            for k in range(5):
                out = jnp.where(lane == k, jnp.sum(acc_w[k, rr, :], axis=1, keepdims=True), out)
            gcw_ref[rr, :] = out


def ssd_bwd(px, cv, y, dy, states, dt, cum, cumt, conv_w, conv_b, dt_bias, a_log, d_skip):
    d_inner, seq = y.shape
    conv_dim = conv_b.shape[0]
    n_heads = dt_bias.shape[0]
    n_chunk = seq // Q
    cw = jnp.concatenate([conv_w.astype(F32), conv_b.astype(F32)[None]], axis=0).T
    hv = jnp.broadcast_to(jnp.stack([dt_bias, -jnp.exp(a_log), d_skip])[:, :, None], (3, n_heads, Q))
    full = lambda s: pl.BlockSpec(s, lambda c: (0,) * len(s))
    tok = lambda rows: pl.BlockSpec((rows, Q), lambda c: (0, n_chunk - 1 - c))
    rows = conv_dim + n_heads
    return pl.pallas_call(
        functools.partial(ssd_bwd_kernel, n_heads, n_chunk),
        grid=(n_chunk,),
        in_specs=[tok(rows), tok(conv_dim), tok(d_inner), tok(d_inner),
                  pl.BlockSpec((1, d_inner, NS), lambda c: (n_chunk - 1 - c, 0, 0)),
                  tok(n_heads), tok(n_heads), pl.BlockSpec((Q, n_heads), lambda c: (n_chunk - 1 - c, 0)),
                  full(cw.shape), full(hv.shape)],
        out_specs=[tok(rows), full((conv_dim, Q)), full((3, n_heads, Q))],
        out_shape=[jax.ShapeDtypeStruct((rows, seq), BF16), jax.ShapeDtypeStruct((conv_dim, Q), F32),
                   jax.ShapeDtypeStruct((3, n_heads, Q), F32)],
        scratch_shapes=[pltpu.VMEM((5, conv_dim, Q), F32), pltpu.VMEM((5, conv_dim, Q), F32), pltpu.VMEM((conv_dim, Q), F32),
                        pltpu.VMEM((d_inner, NS), F32), pltpu.VMEM((Q, Q), F32), pltpu.VMEM((Q, Q), F32),
                        pltpu.VMEM((6, n_heads, Q), F32), pltpu.VMEM((3, n_heads, Q), F32), pltpu.VMEM((2, NS, Q), F32)],
        compiler_params=pltpu.CompilerParams(dimension_semantics=("arbitrary",), vmem_limit_bytes=56 << 20),
        cost_estimate=pl.CostEstimate(flops=60_000_000_000, bytes_accessed=50_000_000, transcendentals=0),
        name="ssd_bwd",
    )(px, cv, y, dy, states, dt, cum, cumt, cw, hv)


def xor_perm(x, axis, bit, size=4):
    return lax.ppermute(x, axis, [(i, i ^ bit) for i in range(size)])


def tie(*xs):
    return lax.optimization_barrier(xs)


def assemble_kernel(order_ref, *refs):
    k = pl.program_id(0)
    for j in range(4):
        @pl.when(k == j)
        def _(j=j):
            refs[4][...] = refs[j][...]


def assemble(pieces, order, axis, n_blk):
    rows, cols = pieces[0].shape
    rb = rows // n_blk

    def in_spec(j):
        return pl.BlockSpec((rb, cols), lambda k, b, o: (jnp.where(k == j, b, jnp.where(k < j, 0, n_blk - 1)), 0))
    if axis == 1:
        shape, out_map = (rows, 4 * cols), lambda k, b, o: (b, o[k])
    else:
        shape, out_map = (4 * rows, cols), lambda k, b, o: (o[k] * n_blk + b, 0)
    return pl.pallas_call(
        assemble_kernel,
        grid_spec=pltpu.PrefetchScalarGridSpec(
            num_scalar_prefetch=1, grid=(4, n_blk), in_specs=[in_spec(j) for j in range(4)],
            out_specs=pl.BlockSpec((rb, cols), out_map)),
        out_shape=jax.ShapeDtypeStruct(shape, pieces[0].dtype),
        compiler_params=pltpu.CompilerParams(dimension_semantics=("arbitrary", "arbitrary"), vmem_limit_bytes=40 << 20),
        cost_estimate=pl.CostEstimate(flops=3_000_000_000, bytes_accessed=16 * rows * cols, transcendentals=0),
        name="assemble",
    )(order, *pieces)


def place_kernel(plan, n_in, order_ref, *refs):
    out_ref, sem = refs[n_in], refs[n_in + 1]
    copies = []
    for k, (layer, base, j) in enumerate(plan):
        rows = refs[k].shape[0]
        lo = pl.multiple_of(base + order_ref[j] * rows, 8)
        copies.append(pltpu.make_async_copy(refs[k], out_ref.at[layer, pl.ds(lo, rows), :], sem.at[k]))
    for c in copies:
        c.start()
    for c in copies:
        c.wait()


def place(blocks, plan, order, shape):
    n_in = len(blocks)
    return pl.pallas_call(
        functools.partial(place_kernel, plan, n_in),
        in_specs=[pl.BlockSpec(memory_space=pltpu.SMEM)] + [pl.BlockSpec(memory_space=pltpu.VMEM)] * n_in,
        out_specs=pl.BlockSpec(memory_space=pl.ANY),
        out_shape=jax.ShapeDtypeStruct(shape, F32),
        scratch_shapes=[pltpu.SemaphoreType.DMA((n_in,))],
        compiler_params=pltpu.CompilerParams(vmem_limit_bytes=40 << 20),
        name="place",
    )(order, *blocks)


def dot_f32(a, b, dims):
    return lax.dot_general(a, b, (dims, ((), ())), preferred_element_type=F32)


def pre_norm(u_rows, norm_w):
    rows_f = u_rows.astype(F32)
    inv_rms = lax.rsqrt(jnp.mean(jnp.square(rows_f), axis=-1, keepdims=True) + NORM_EPS)
    return (rows_f * inv_rms * norm_w).astype(BF16)


def pre_norm_bwd(u_rows, norm_w, d_h):
    rows_f = u_rows.astype(F32)
    inv_rms = lax.rsqrt(jnp.mean(jnp.square(rows_f), axis=-1, keepdims=True) + NORM_EPS)
    d_f = d_h.astype(F32)
    unit = rows_f * inv_rms
    g_w = jnp.sum(d_f * unit, axis=0)
    d_unit = d_f * norm_w
    d_rows = inv_rms * (d_unit - unit * jnp.mean(d_unit * unit, axis=-1, keepdims=True))
    return d_rows.astype(BF16), g_w


def solution(mesh):
    dp_size = mesh.shape['dp']
    fsdp_size = mesh.shape['fsdp']
    act_spec = P(('dp', 'fsdp'), None, None)
    weight_specs = (P(None, 'fsdp'), P(None, 'fsdp', None), P(None, None, 'fsdp'), P(None, 'fsdp'), P(None, 'fsdp'), P(None, 'fsdp'), P(None, 'fsdp'), P(None, 'fsdp'), P(None, 'fsdp', None))

    def per_device(u_loc, g_loc, norm_w, w_in, conv_w, conv_b, dt_bias, a_log, d_skip, gate_w, w_out):
        batch_tot = u_loc.shape[0] * dp_size * fsdp_size
        u_in, grad_out = u_loc[0], g_loc[0]
        me = lax.axis_index('fsdp')
        dp_me = lax.axis_index('dp')
        core = me % 2
        x_pos = me // 2
        order_f = jnp.stack([me, me ^ 1, me ^ 2, me ^ 3]).astype(jnp.int32)
        order_d = jnp.stack([dp_me, dp_me ^ 1, dp_me ^ 2, dp_me ^ 3]).astype(jnp.int32)
        d_inner = gate_w.shape[1] * fsdp_size
        d_model = norm_w.shape[1] * fsdp_size
        d_piece = d_model // 4
        o_piece = d_inner // 4
        w_in_t = jnp.transpose(w_in, (0, 2, 1))

        small_pieces = (norm_w, conv_w, conv_b, dt_bias, a_log, d_skip, gate_w)
        sizes = [p.size for p in small_pieces]
        flat = jnp.concatenate([p.astype(F32).reshape(-1) for p in small_pieces])
        flat_rel = [flat] + [xor_perm(flat, 'fsdp', bit) for bit in (1, 2, 3)]

        pieces = [(w_in_t[n, d_inner:], w_in_t[n, :d_inner], w_out[n]) for n in range(2)]
        far = [[xor_perm(p, 'fsdp', 2) for p in pieces[n]] for n in range(2)]
        near = [[xor_perm(p, 'fsdp', 1) for p in pieces[n]] for n in range(2)]
        AXES, BLKS = (1, 1, 0), (2, 2, 2)

        flat_all = jnp.take(jnp.stack(flat_rel), order_f, axis=0)
        smalls = []
        lo = 0
        for p, size in zip(small_pieces, sizes):
            part = flat_all[:, lo:lo + size].reshape((fsdp_size,) + p.shape)
            smalls.append(jnp.moveaxis(part, 0, -2).reshape(p.shape[:-1] + (fsdp_size * p.shape[-1],)))
            lo += size
        norm_f, conv_f, convb_f, dtb_f, alog_f, dskip_f, gate_f = smalls

        def diag_of(n, k):
            return xor_perm(far[n][k], 'fsdp', 1)

        def join(n, k, diag):
            return assemble([pieces[n][k], near[n][k], far[n][k], diag], order_f, AXES[k], BLKS[k])

        def proj(h, w_t):
            return dot_f32(w_t, h, ((1,), (1,))).astype(BF16)

        def mixer(pz, px, n):
            return ssd_fwd(pz, px, conv_f[n], convb_f[n], dtb_f[n], alog_f[n], dskip_f[n], gate_f[n])

        def out_proj(u_rows, n_t, w_o):
            return (u_rows.astype(F32) + dot_f32(n_t, w_o, ((0,), (0,)))).astype(BF16)

        h0 = pre_norm(u_in, norm_f[0])
        wx0 = join(0, 0, diag_of(0, 0))
        px0 = proj(h0, wx0)
        far[0][1], px0 = tie(far[0][1], px0)
        wz0 = join(0, 1, diag_of(0, 1))
        pz0 = proj(h0, wz0)
        f0 = mixer(pz0, px0, 0)
        held = tie(f0[0], far[0][2], far[1][0], far[1][1])
        f0 = (held[0],) + tuple(f0[1:])
        far[0][2], far[1][0], far[1][1] = held[1:]
        diags = (diag_of(0, 2), diag_of(1, 0), diag_of(1, 1))
        wo0 = join(0, 2, diags[0])
        hidden = out_proj(u_in, f0[0], wo0)
        h1 = pre_norm(hidden, norm_f[1])
        wx1 = join(1, 0, diags[1])
        px1 = proj(h1, wx1)
        wz1 = join(1, 1, diags[2])
        pz1 = proj(h1, wz1)
        f1 = mixer(pz1, px1, 1)
        held = tie(f1[0], far[1][2])
        f1 = (held[0],) + tuple(f1[1:])
        far[1][2] = held[1]
        wo1 = join(1, 2, diag_of(1, 2))

        saved = ((u_in, h0, px0, pz0) + tuple(f0), (hidden, h1, px1, pz1) + tuple(f1))
        big = ((wx0, wz0, wo0), (wx1, wz1, wo1))

        def reduction(make, rows):
            sent = (make(1 - x_pos, 1 - core), make(x_pos, 1 - core))
            recv = yield sent, [xor_perm(s, 'fsdp', 1) for s in sent]
            away = make(1 - x_pos, core) + recv[0]
            far_in = xor_perm(away, 'fsdp', 2)
            part = make(x_pos, core) + recv[1]
            recv = yield (away, part), [far_in]
            piece = part + recv[0]
            quarters = piece.reshape(4, rows // 4, piece.shape[1])
            sent = [lax.dynamic_index_in_dim(quarters, dp_me ^ bit, 0, False) for bit in (3, 1, 2)]
            own = lax.dynamic_index_in_dim(quarters, dp_me, 0, False)
            recv = yield tuple(sent) + (own,), [xor_perm(s, 'dp', bit) for s, bit in zip(sent, (3, 1, 2))]
            total = own.astype(F32) + recv[0].astype(F32) + recv[1].astype(F32) + recv[2].astype(F32)
            got = yield (total,), [xor_perm(total, 'dp', bit) for bit in (3, 1, 2)]
            return [total, got[1], got[2], got[0]]

        def small_reduction(vec):
            for axis, bit in (('fsdp', 1), ('fsdp', 2), ('dp', 1), ('dp', 2)):
                recv = yield (vec,), [xor_perm(vec, axis, bit)]
                vec = vec + recv[0]
            return vec

        live = []
        done = {}

        def launch(name, gen):
            sends, recvs = next(gen)
            live.append([name, gen, recvs])
            return list(sends)

        def advance(*anchors):
            if anchors:
                flat_in = [r for item in live for r in item[2]]
                held = tie(*anchors, *flat_in)
                anchors, flat_in = list(held[:len(anchors)]), list(held[len(anchors):])
                for item in live:
                    item[2] = [flat_in.pop(0) for _ in item[2]]
            sends = []
            for item in list(live):
                try:
                    new_sends, item[2] = item[1].send(item[2])
                    sends.extend(new_sends)
                except StopIteration as stop:
                    done[item[0]] = stop.value
                    live.remove(item)
            return anchors, sends

        def backward(d_out, n, last):
            u_rows, h, px, pz, n_t, y, st, cv, r, dt, cum, cumt = saved[n]
            w_x, w_z, w_o = big[n]

            def make_out(xp, c):
                rows = lax.dynamic_slice_in_dim(n_t, (2 * xp + c) * o_piece, o_piece, 0)
                return (dot_f32(rows, d_out, ((1,), (0,))) / batch_tot).astype(BF16)

            def make_in(d_t):
                def make(xp, c):
                    cols = lax.dynamic_slice_in_dim(h, (2 * xp + c) * d_piece, d_piece, 1)
                    return (dot_f32(d_t, cols, ((1,), (0,))) / batch_tot).astype(BF16)
                return make
            sends = launch(('o', n), reduction(make_out, o_piece))
            dn = proj(d_out, w_o)
            (dn,), more = advance(dn)
            dn = tie(dn, *sends, *more)[0]
            dz, dy, gg = gate_bwd(pz, y, cv, dn, r, gate_f[n], dskip_f[n])
            (dz, dy), more = advance(dz, dy)
            sends = launch(('z', n), reduction(make_in(dz), dz.shape[0]))
            d_h = dot_f32(dz, w_z, ((0,), (0,)))
            dy = tie(dy, d_h, *sends, *more)[0]
            dpx, gcw, gh = ssd_bwd(px, cv, y, dy, st, dt, cum, cumt, conv_f[n], convb_f[n], dtb_f[n], alog_f[n], dskip_f[n])
            (dpx,), more = advance(dpx)
            sends = launch(('x', n), reduction(make_in(dpx), dpx.shape[0]))
            d_h = (d_h + dot_f32(dpx, w_x, ((0,), (0,)))).astype(BF16)
            d_norm, g_norm = pre_norm_bwd(u_rows, norm_f[n], d_h)
            d_u = (d_out.astype(F32) + d_norm.astype(F32)).astype(BF16)
            gh = jnp.sum(gh, axis=-1) / batch_tot
            half = lambda g: (g / batch_tot).astype(BF16).astype(F32)
            small = (half(g_norm), half(gcw[:, :4].T), half(gcw[:, 4]), gh[0], gh[1], gh[2], half(jnp.sum(gg, axis=-1)))
            sends += launch(('s', n), small_reduction(jnp.concatenate([s.reshape(-1) for s in small])))
            if not last:
                d_u = tie(d_u, *sends, *more)[0]
                (d_u,), more = advance(d_u)
                d_u = tie(d_u, *more)[0]
            return d_u

        d_out1 = tie(grad_out, f1[0])[0]
        d_hidden = backward(d_out1, 1, False)
        d_u = backward(d_hidden, 0, True)
        out = out_proj(hidden, f1[0], wo1)
        while live:
            advance()

        g_small = []
        lo = 0
        for p in small_pieces:
            size = p.size * fsdp_size // 2
            whole = jnp.stack([done[('s', n)][lo:lo + size] for n in range(2)]).reshape(p.shape[:-1] + (fsdp_size * p.shape[-1],))
            g_small.append(lax.dynamic_slice_in_dim(whole, me * p.shape[-1], p.shape[-1], p.ndim - 1))
            lo += size

        def finish(parts, shape):
            blocks, plan = [], []
            for n in (1, 0):
                base = 0
                for part in parts:
                    for j, blk in enumerate(done[(part, n)]):
                        blocks.append(blk)
                        plan.append((n, base, j))
                    base += 4 * blk.shape[0]
            return place(blocks, plan, order_d, shape)
        g_out = finish('o', w_out.shape)
        g_in = jnp.transpose(finish('zx', w_in_t.shape), (0, 2, 1))
        g_norm, g_conv, g_convb, g_dtb, g_alog, g_dskip, g_gate = g_small
        return out[None], d_u[None], g_norm, g_in, g_conv, g_convb, g_dtb, g_alog, g_dskip, g_gate, g_out

    return jax.shard_map(per_device, mesh=mesh, in_specs=(act_spec, act_spec) + weight_specs, out_specs=(act_spec, act_spec) + weight_specs, check_vma=False)
```

```python
import functools
import jax
import jax.numpy as jnp
from jax import lax
from jax.sharding import PartitionSpec as P
from jax.experimental import pallas as pl
from jax.experimental.pallas import tpu as pltpu

F32 = jnp.float32
BF16 = jnp.bfloat16
NORM_EPS = 1e-5
LOG2E = 1.4426950408889634
Q = 128
HP = 64
NS = 128
NN = (((1,), (0,)), ((), ()))
NT = (((1,), (1,)), ((), ()))
TN = (((0,), (0,)), ((), ()))


def mm(a, b, dims=NN):
    return lax.dot_general(a, b, dims, preferred_element_type=F32)


def sigm(v):
    return 0.5 * jnp.tanh(0.5 * v) + 0.5


def blocks_of(total, size):
    return [(lo, min(size, total - lo)) for lo in range(0, total, size)]


def row_loop(total, size):
    def run(body):
        @pl.loop(0, total // size)
        def _(i):
            body(pl.ds(pl.multiple_of(i * size, size), size))
    return run


def whole(arr_shape):
    zeros = (0,) * len(arr_shape)
    return pl.BlockSpec(arr_shape, lambda c: zeros)


def by_token(rows, n_rev=None):
    return pl.BlockSpec((rows, Q), lambda c: (0, c if n_rev is None else n_rev - c))


def by_chunk(rows, n_rev=None):
    return pl.BlockSpec((None, rows, Q), lambda c: (c if n_rev is None else n_rev - c, 0, 0))


def params(vmem=56 << 20):
    return pltpu.CompilerParams(dimension_semantics=("arbitrary",), vmem_limit_bytes=vmem)


def cost(flops):
    return pl.CostEstimate(flops=flops, bytes_accessed=40_000_000, transcendentals=0)


SCAN = tuple(2 ** e for e in range(7))


def dt_kernel(pdt_ref, hv_ref, dt_ref, cum_ref, cumt_ref):
    n_heads, seq = dt_ref.shape
    lane = lane_iota(n_heads)
    cols = [slice(lo, lo + Q) for lo in range(0, seq, Q)]
    accs = []
    for cc in cols:
        raw = pdt_ref[:, cc].astype(F32) + hv_ref[0]
        dt = jnp.maximum(raw, 0.0) + jnp.log1p(jnp.exp(-jnp.abs(raw)))
        dt_ref[:, cc] = dt
        accs.append(dt * hv_ref[1])
    for k in SCAN:
        accs = [acc + jnp.where(lane >= k, pltpu.roll(acc, k, 1), 0.0) for acc in accs]
    for cc, acc in zip(cols, accs):
        cum_ref[:, cc] = acc
        cumt_ref[cc, :] = jnp.transpose(acc)


def lane_iota(rows):
    return lax.broadcasted_iota(jnp.int32, (rows, Q), 1)


EXPC, EXPE, EXPT, CUM2, DT, SKIP, N_ROWS = range(7)
TAPS = 4
GRP = 4
PER = 4
RB = 256


def causal_mask():
    return lax.broadcasted_iota(jnp.int32, (Q, Q), 0) <= lax.broadcasted_iota(jnp.int32, (Q, Q), 1)


def fill_rows(rows_s, cum, dt, skip):
    tot = jnp.broadcast_to(cum[:, Q - 1:Q], cum.shape)
    for a, v in ((EXPC, jnp.exp(cum)), (EXPE, jnp.exp(tot - cum)), (EXPT, jnp.exp(tot)), (CUM2, cum * LOG2E), (DT, dt), (SKIP, skip)):
        rows_s[a] = v


def fold8(v):
    parts = [v[lo:lo + 8, :] for lo in range(0, v.shape[0], 8)]
    while len(parts) > 1:
        parts = [a + b for a, b in zip(parts[::2], parts[1::2])]
    return parts[0]


def ssd_fwd_kernel(n_heads, pz_ref, px_ref, cw_ref, gw_ref, hv_ref, dt_ref, cum_ref, cumt_ref,
                   n_ref, y_ref, s_ref, cv_ref, r_ref,
                   wb, gb, xprev, xs, vs, gt_s, st, rows_s):
    step = pl.program_id(0)
    d_inner = n_heads * HP
    conv_dim = d_inner + 2 * NS

    @pl.when(step == 0)
    def _():
        @row_loop(conv_dim, RB)
        def _(rr):
            for k in range(TAPS + 1):
                wb[k, rr, :] = jnp.broadcast_to(cw_ref[rr, k:k + 1], (RB, Q))
            xprev[rr, :] = jnp.zeros((RB, Q), BF16)

        @row_loop(d_inner, RB)
        def _(rr):
            gb[rr, :] = jnp.broadcast_to(gw_ref[rr, 0:1], (RB, Q))
            st[rr, :] = jnp.zeros((RB, NS), F32)

    @row_loop(conv_dim, RB)
    def _(rr):
        lane = lane_iota(RB)
        raw = px_ref[rr, :]
        x = raw.astype(F32)
        xp = xprev[rr, :].astype(F32)
        xprev[rr, :] = raw
        shifted = [pltpu.roll(jnp.where(lane >= Q - j, xp, x), j, 1) for j in range(1, TAPS)]
        acc = wb[TAPS, rr, :] + wb[TAPS - 1, rr, :] * x
        for j in range(1, TAPS):
            acc = acc + wb[TAPS - 1 - j, rr, :] * shifted[j - 1]
        cv_ref[rr, :] = acc
        xs[rr, :] = acc * sigm(acc)

    bt = xs[d_inner:d_inner + NS, :].astype(BF16)
    ct = xs[d_inner + NS:, :].astype(BF16)
    gt_s[...] = jnp.where(causal_mask(), mm(bt, ct, TN), 0.0)
    fill_rows(rows_s, cum_ref[...], dt_ref[...], hv_ref[2])
    cumt = cumt_ref[...] * LOG2E

    ssq = jnp.zeros((8, Q), F32)
    for lo in range(0, n_heads, GRP):
        gg = slice(lo * HP, (lo + GRP) * HP)
        st_g = st[gg, :]
        s_ref[gg, :] = st_g
        yoff = mm(st_g.astype(BF16), ct)
        xe = []
        for k in range(GRP):
            h = lo + k
            row = lambda a: rows_s[a, h:h + 1, :]
            hh = slice(h * HP, (h + 1) * HP)
            x = xs[hh, :]
            xdt = x * row(DT)
            gap = row(CUM2) - cumt[:, h:h + 1]
            mt = (gt_s[...] * jnp.exp2(jnp.minimum(gap, 0.0))).astype(BF16)
            y = mm(xdt.astype(BF16), mt) + yoff[k * HP:(k + 1) * HP, :] * row(EXPC)
            y_ref[hh, :] = y
            z = pz_ref[hh, :].astype(F32)
            v = (y + row(SKIP) * x) * (z * sigm(z))
            vs[hh, :] = v
            ssq = ssq + fold8(v * v)
            xe.append((xdt * row(EXPE)).astype(BF16))
        upd = mm(jnp.concatenate(xe, axis=0), bt, NT)
        for k in range(GRP):
            h = lo + k
            hh = slice(h * HP, (h + 1) * HP)
            st[hh, :] = st[hh, :] * rows_s[EXPT, h:h + 1, :] + upd[k * HP:(k + 1) * HP, :]

    r = lax.rsqrt(jnp.sum(ssq, axis=0, keepdims=True) / d_inner + NORM_EPS)
    r_ref[:, :] = r

    @row_loop(d_inner, RB)
    def _(rr):
        n_ref[rr, :] = (vs[rr, :] * r * gb[rr, :]).astype(BF16)


def head_params(dt_bias, a_log, d_skip):
    return jnp.broadcast_to(jnp.stack([dt_bias, -jnp.exp(a_log), d_skip])[:, :, None], (3, dt_bias.shape[0], Q))


def conv_params(conv_w, conv_b):
    return jnp.concatenate([conv_w.astype(F32), conv_b.astype(F32)[None]], axis=0).T


def ssd_dt(px, hv):
    n_heads = hv.shape[1]
    seq = px.shape[1]
    last = px.shape[0] // n_heads - 1
    shapes = [(n_heads, seq), (n_heads, seq), (seq, n_heads)]
    return pl.pallas_call(
        dt_kernel, grid=(1,),
        in_specs=[pl.BlockSpec((n_heads, seq), lambda c: (last, c)), whole(hv.shape)],
        out_specs=[whole(s) for s in shapes], out_shape=[jax.ShapeDtypeStruct(s, F32) for s in shapes],
        compiler_params=params(16 << 20), name="ssd_dt",
    )(px, hv)


def ssd_fwd(pz, px, cw, gw, hv):
    d_inner, seq = pz.shape
    conv_dim = cw.shape[0]
    n_heads = hv.shape[1]
    n_chunk = seq // Q
    dt, cum, cumt = ssd_dt(px, hv)
    f32s = lambda *s: jax.ShapeDtypeStruct(s, F32)
    outs = pl.pallas_call(
        functools.partial(ssd_fwd_kernel, n_heads),
        grid=(n_chunk,),
        in_specs=[by_token(d_inner), by_token(px.shape[0]), whole(cw.shape), whole(gw.shape), whole(hv.shape),
                  by_token(n_heads), by_token(n_heads), pl.BlockSpec((Q, n_heads), lambda c: (c, 0))],
        out_specs=[by_token(d_inner), by_chunk(d_inner), by_chunk(d_inner), by_chunk(conv_dim), by_token(1)],
        out_shape=[jax.ShapeDtypeStruct((d_inner, seq), BF16), f32s(n_chunk, d_inner, Q), f32s(n_chunk, d_inner, NS), f32s(n_chunk, conv_dim, Q), f32s(1, seq)],
        scratch_shapes=[pltpu.VMEM((TAPS + 1, conv_dim, Q), F32), pltpu.VMEM((d_inner, Q), F32), pltpu.VMEM((conv_dim, Q), BF16),
                        pltpu.VMEM((conv_dim, Q), F32), pltpu.VMEM((d_inner, Q), F32), pltpu.VMEM((Q, Q), F32),
                        pltpu.VMEM((d_inner, NS), F32), pltpu.VMEM((N_ROWS, n_heads, Q), F32)],
        compiler_params=params(), cost_estimate=cost(30_000_000_000), name="ssd_fwd",
    )(pz, px, cw, gw, hv, dt, cum, cumt)
    return tuple(outs) + (dt, cum, cumt)


def gate_bwd_kernel(n_heads, pz_ref, y_ref, cv_ref, dn_ref, r_ref, gw_ref, hv_ref,
                    dz_ref, dy_ref, gg_ref, gb, sk):
    step = pl.program_id(0)
    d_inner = n_heads * HP

    @pl.when(step == 0)
    def _():
        @row_loop(d_inner, RB)
        def _(rr):
            gb[rr, :] = jnp.broadcast_to(gw_ref[rr, 0:1], (RB, Q))
            gg_ref[rr, :] = jnp.zeros((RB, Q), F32)
        sk[...] = hv_ref[2]
    r = r_ref[:, :]
    per = PER

    def rows(i):
        return pl.ds(pl.multiple_of(i * (per * HP), per * HP), per * HP)

    def pass1(i, acc):
        rr = rows(i)
        cv = cv_ref[rr, :]
        x = cv * sigm(cv)
        skip = jnp.concatenate([jnp.broadcast_to(sk[pl.ds(i * per + k, 1), :], (HP, Q)) for k in range(per)], axis=0)
        yf = y_ref[rr, :] + skip * x
        dy_ref[rr, :] = yf
        z = pz_ref[rr, :].astype(F32)
        t = dn_ref[rr, :].astype(F32) * (yf * (z * sigm(z)) * r)
        gg_ref[rr, :] = gg_ref[rr, :] + t
        return acc + fold8(t * gb[rr, :])
    acc = lax.fori_loop(0, n_heads // per, pass1, jnp.zeros((8, Q), F32))
    mean = jnp.sum(acc, axis=0, keepdims=True) / d_inner

    @pl.loop(0, n_heads // per)
    def _(i):
        rr = rows(i)
        z = pz_ref[rr, :].astype(F32)
        yf = dy_ref[rr, :]
        sg = sigm(z)
        sl = z * sg
        dv = r * (dn_ref[rr, :].astype(F32) * gb[rr, :] - (yf * sl * r) * mean)
        dy_ref[rr, :] = dv * sl
        dz_ref[rr, :] = (dv * yf * (sg + sl * (1.0 - sg))).astype(BF16)


def gate_bwd(pz, y, cv, dn, r, gw, hv):
    d_inner, seq = pz.shape
    n_heads = hv.shape[1]
    return pl.pallas_call(
        functools.partial(gate_bwd_kernel, n_heads),
        grid=(seq // Q,),
        in_specs=[by_token(d_inner), by_chunk(d_inner), by_chunk(d_inner), by_token(d_inner), by_token(1), whole(gw.shape), whole(hv.shape)],
        out_specs=[by_token(d_inner), by_chunk(d_inner), whole((d_inner, Q))],
        out_shape=[jax.ShapeDtypeStruct((d_inner, seq), BF16), jax.ShapeDtypeStruct(y.shape, F32),
                   jax.ShapeDtypeStruct((d_inner, Q), F32)],
        scratch_shapes=[pltpu.VMEM((d_inner, Q), F32), pltpu.VMEM((n_heads, Q), F32)],
        compiler_params=params(), cost_estimate=cost(15_000_000_000), name="gate_bwd",
    )(pz, y, cv, dn, r, gw, hv)


def ssd_bwd_kernel(n_heads, n_chunk, px_ref, cv_ref, y_ref, dy_ref, s_ref, dt_ref, cum_ref, cumt_ref, cw_ref, hv_ref,
                   dpx_ref, gcw_ref, gh_ref,
                   wb, acc_w, dbuf, ds, gt_s, dg_s, rows_s, red_s, dbc):
    step = pl.program_id(0)
    d_inner = n_heads * HP
    conv_dim = d_inner + 2 * NS

    @pl.when(step == 0)
    def _():
        @row_loop(conv_dim, RB)
        def _(rr):
            for k in range(TAPS + 1):
                wb[k, rr, :] = jnp.broadcast_to(cw_ref[rr, k:k + 1], (RB, Q))
                acc_w[k, rr, :] = jnp.zeros((RB, Q), F32)
            dbuf[1, rr, :] = jnp.zeros((RB, Q), F32)

        @row_loop(d_inner, RB)
        def _(rr):
            ds[rr, :] = jnp.zeros((RB, NS), F32)
        gh_ref[...] = jnp.zeros(gh_ref.shape, F32)
    now = lax.rem(step, 2)
    later = 1 - now

    def act(cv):
        sg = sigm(cv)
        a = cv * sg
        return a, sg + a * (1.0 - sg)

    br = slice(d_inner, d_inner + NS)
    cr = slice(d_inner + NS, conv_dim)
    b_act, b_der = act(cv_ref[br, :])
    c_act, c_der = act(cv_ref[cr, :])
    bt = b_act.astype(BF16)
    ct = c_act.astype(BF16)
    gt_s[...] = jnp.where(causal_mask(), mm(bt, ct, TN), 0.0)
    fill_rows(rows_s, cum_ref[...], dt_ref[...], hv_ref[2])
    cumt = cumt_ref[...] * LOG2E
    d_a_sum, d_cum, d_dt = range(3)

    for lo in range(0, n_heads, GRP):
        gg = slice(lo * HP, (lo + GRP) * HP)
        ds_b = ds[gg, :].astype(BF16)
        sp_b = s_ref[gg, :].astype(BF16)
        dsb = mm(ds_b, bt)
        dye, xde, dgs = [], [], []
        for k in range(GRP):
            h = lo + k
            hh = slice(h * HP, (h + 1) * HP)
            kk = slice(k * HP, (k + 1) * HP)
            row = lambda a: rows_s[a, h:h + 1, :]
            total = lambda v: jnp.sum(v, axis=0, keepdims=True)
            x, der = act(cv_ref[hh, :])
            xdt = x * row(DT)
            xdt_b = xdt.astype(BF16)
            dy = dy_ref[hh, :]
            dy_b = dy.astype(BF16)
            dmt = mm(xdt_b, dy_b, TN)
            dec = jnp.exp2(jnp.minimum(row(CUM2) - cumt[:, h:h + 1], 0.0))
            mt = (gt_s[...] * dec).astype(BF16)
            dgs.append(dmt * dec)
            t2 = dsb[kk, :] * row(EXPE)
            dxdt = mm(dy_b, mt, NT) + t2
            xdt_r = xdt_b.astype(F32)
            red_s[d_dt, h:h + 1, :] = total(dxdt * x)
            red_s[d_cum, h:h + 1, :] = total(dy_b.astype(F32) * y_ref[hh, :] - xdt_r * dxdt)
            red_s[d_a_sum, h:h + 1, :] = total(xdt_r * t2 + row(EXPT) * (ds[hh, :] * s_ref[hh, :]))
            gh_ref[2, h:h + 1, :] = gh_ref[2, h:h + 1, :] + total(dy * x)
            dye.append((dy * row(EXPC)).astype(BF16))
            xde.append((xdt * row(EXPE)).astype(BF16))
            dbuf[now, hh, :] = (dxdt * row(DT) + row(SKIP) * dy) * der
        dye = jnp.concatenate(dye, axis=0)
        xde = jnp.concatenate(xde, axis=0)
        dg = (dgs[0] + dgs[1]) + (dgs[2] + dgs[3])
        d_b, d_c = mm(ds_b, xde, TN), mm(sp_b, dye, TN)
        if lo == 0:
            dg_s[...], dbc[0], dbc[1] = dg, d_b, d_c
        else:
            dg_s[...] = dg_s[...] + dg
            dbc[0] = dbc[0] + d_b
            dbc[1] = dbc[1] + d_c
        upd = mm(dye, ct, NT)
        for k in range(GRP):
            h = lo + k
            hh = slice(h * HP, (h + 1) * HP)
            ds[hh, :] = ds[hh, :] * rows_s[EXPT, h:h + 1, :] + upd[k * HP:(k + 1) * HP, :]

    dg = jnp.where(causal_mask(), dg_s[...], 0.0).astype(BF16)
    dbuf[now, br, :] = (dbc[0] + mm(ct, dg, NT)) * b_der
    dbuf[now, cr, :] = (dbc[1] + mm(bt, dg)) * c_der

    lane = lane_iota(n_heads)
    suf = red_s[d_cum]
    for k in SCAN:
        suf = suf + jnp.where(lane < Q - k, pltpu.roll(suf, Q - k, 1), 0.0)
    d_a = suf + jnp.broadcast_to(jnp.sum(red_s[d_a_sum], axis=1, keepdims=True), (n_heads, Q))
    raw_dt = px_ref[conv_dim:, :].astype(F32) + hv_ref[0]
    d_raw = (red_s[d_dt] + d_a * hv_ref[1]) * sigm(raw_dt)
    dpx_ref[conv_dim:, :] = d_raw.astype(BF16)
    gh_ref[0] = gh_ref[0] + d_raw
    gh_ref[1] = gh_ref[1] + d_a * dt_ref[...] * hv_ref[1]

    @row_loop(conv_dim, RB)
    def _(rr):
        lane = lane_iota(RB)
        raw = px_ref[rr, :].astype(F32)
        nxt = dbuf[later, rr, :]
        dcv = dbuf[now, rr, :]
        shifted = [pltpu.roll(jnp.where(lane < j, nxt, dcv), Q - j, 1) for j in range(1, TAPS)]
        acc_w[TAPS, rr, :] = acc_w[TAPS, rr, :] + dcv
        dx = 0.0
        for j, sh in enumerate([dcv] + shifted):
            tap = TAPS - 1 - j
            acc_w[tap, rr, :] = acc_w[tap, rr, :] + sh * raw
            dx = dx + wb[tap, rr, :] * sh
        dpx_ref[rr, :] = dx.astype(BF16)

    @pl.when(step == n_chunk - 1)
    def _():
        @row_loop(conv_dim, RB)
        def _(rr):
            lane = lane_iota(RB)
            out = jnp.zeros((RB, Q), F32)
            for k in range(TAPS + 1):
                out = jnp.where(lane == k, jnp.sum(acc_w[k, rr, :], axis=1, keepdims=True), out)
            gcw_ref[rr, :] = out


def ssd_bwd(px, cv, y, dy, states, dt, cum, cumt, cw, hv):
    n_chunk, d_inner, _ = y.shape
    conv_dim, seq = cw.shape[0], px.shape[1]
    n_heads = hv.shape[1]
    rev = n_chunk - 1
    rows = px.shape[0]
    tok = lambda n: by_token(n, rev)
    chunk = lambda n: by_chunk(n, rev)
    taps = pltpu.VMEM((TAPS + 1, conv_dim, Q), F32)
    square = pltpu.VMEM((Q, Q), F32)
    return pl.pallas_call(
        functools.partial(ssd_bwd_kernel, n_heads, n_chunk),
        grid=(n_chunk,),
        in_specs=[tok(rows), chunk(conv_dim), chunk(d_inner), chunk(d_inner), chunk(d_inner),
                  tok(n_heads), tok(n_heads), pl.BlockSpec((Q, n_heads), lambda c: (rev - c, 0)),
                  whole(cw.shape), whole(hv.shape)],
        out_specs=[tok(rows), whole((conv_dim, Q)), whole(hv.shape)],
        out_shape=[jax.ShapeDtypeStruct((rows, seq), BF16), jax.ShapeDtypeStruct((conv_dim, Q), F32),
                   jax.ShapeDtypeStruct(hv.shape, F32)],
        scratch_shapes=[taps, taps, pltpu.VMEM((2, conv_dim, Q), F32), pltpu.VMEM((d_inner, NS), F32), square, square,
                        pltpu.VMEM((N_ROWS, n_heads, Q), F32), pltpu.VMEM((3, n_heads, Q), F32), pltpu.VMEM((2, NS, Q), F32)],
        compiler_params=params(), cost_estimate=cost(60_000_000_000), name="ssd_bwd",
    )(px, cv, y, dy, states, dt, cum, cumt, cw, hv)


def xor_perm(x, axis, bit, size=4):
    return lax.ppermute(x, axis, [(i, i ^ bit) for i in range(size)])


def tie(*xs):
    return lax.optimization_barrier(xs)


def assemble_kernel(starts, n_src, order_ref, *refs):
    k = pl.program_id(0)
    ends = starts[1:] + (pl.num_programs(0),)
    for j in range(n_src):
        @pl.when((k >= starts[j]) & (k < ends[j]))
        def _(j=j):
            refs[n_src][...] = refs[j][...]


def assemble(sources, where, axis, rb):
    cols = sources[0].shape[1]
    counts = [src.shape[0] // rb for src in sources]
    starts = tuple(sum(counts[:j]) for j in range(len(counts)))
    n_steps = sum(counts)
    per = n_steps // 4

    def in_spec(j):
        return pl.BlockSpec((rb, cols), lambda k, o: (jnp.clip(k - starts[j], 0, counts[j] - 1), 0))
    if axis:
        shape, out_map = (per * rb, 4 * cols), lambda k, o: (o[k, 1], o[k, 0])
    else:
        shape, out_map = (n_steps * rb, cols), lambda k, o: (o[k, 0] * per + o[k, 1], 0)
    return pl.pallas_call(
        functools.partial(assemble_kernel, starts, len(sources)),
        grid_spec=pltpu.PrefetchScalarGridSpec(
            num_scalar_prefetch=1, grid=(n_steps,), in_specs=[in_spec(j) for j in range(len(sources))],
            out_specs=pl.BlockSpec((rb, cols), out_map)),
        out_shape=jax.ShapeDtypeStruct(shape, sources[0].dtype),
        compiler_params=params(40 << 20), cost_estimate=cost(3_000_000_000), name="assemble",
    )(where, *sources)


def place_kernel(plan, n_in, order_ref, *refs):
    out_ref, sem = refs[n_in], refs[n_in + 1]
    copies = []
    for k, (layer, base, j) in enumerate(plan):
        rows = refs[k].shape[0]
        lo = pl.multiple_of(base + order_ref[j] * rows, 8)
        copies.append(pltpu.make_async_copy(refs[k], out_ref.at[layer, pl.ds(lo, rows), :], sem.at[k]))
    for c in copies:
        c.start()
    for c in copies:
        c.wait()


def place(blocks, plan, order, shape):
    n_in = len(blocks)
    return pl.pallas_call(
        functools.partial(place_kernel, plan, n_in),
        in_specs=[pl.BlockSpec(memory_space=pltpu.SMEM)] + [pl.BlockSpec(memory_space=pltpu.VMEM)] * n_in,
        out_specs=pl.BlockSpec(memory_space=pl.ANY),
        out_shape=jax.ShapeDtypeStruct(shape, F32),
        scratch_shapes=[pltpu.SemaphoreType.DMA((n_in,))],
        compiler_params=pltpu.CompilerParams(vmem_limit_bytes=40 << 20),
        name="place",
    )(order, *blocks)


def dot_f32(a, b, dims):
    return lax.dot_general(a, b, (dims, ((), ())), preferred_element_type=F32)


def pre_norm(u_rows, norm_w):
    rows_f = u_rows.astype(F32)
    inv_rms = lax.rsqrt(jnp.mean(jnp.square(rows_f), axis=0, keepdims=True) + NORM_EPS)
    return (rows_f * inv_rms * norm_w[:, None]).astype(BF16)


def pre_norm_bwd(u_rows, norm_w, d_h):
    rows_f = u_rows.astype(F32)
    inv_rms = lax.rsqrt(jnp.mean(jnp.square(rows_f), axis=0, keepdims=True) + NORM_EPS)
    d_f = d_h.astype(F32)
    unit = rows_f * inv_rms
    g_w = jnp.sum(d_f * unit, axis=1)
    d_unit = d_f * norm_w[:, None]
    d_rows = inv_rms * (d_unit - unit * jnp.mean(d_unit * unit, axis=0, keepdims=True))
    return d_rows.astype(BF16), g_w


def solution(mesh):
    dp_size = mesh.shape['dp']
    fsdp_size = mesh.shape['fsdp']
    act_spec = P(('dp', 'fsdp'), None, None)
    weight_specs = (P(None, 'fsdp'), P(None, 'fsdp', None), P(None, None, 'fsdp'), P(None, 'fsdp'), P(None, 'fsdp'), P(None, 'fsdp'), P(None, 'fsdp'), P(None, 'fsdp'), P(None, 'fsdp', None))

    def per_device(u_loc, g_loc, norm_w, w_in, conv_w, conv_b, dt_bias, a_log, d_skip, gate_w, w_out):
        batch_tot = u_loc.shape[0] * dp_size * fsdp_size
        u_in, grad_out = u_loc[0].T, g_loc[0].T
        me = lax.axis_index('fsdp')
        dp_me = lax.axis_index('dp')
        core = me % 2
        x_pos = me // 2
        order_f = jnp.stack([me, me ^ 1, me ^ 2, me ^ 3]).astype(jnp.int32)
        order_d = jnp.stack([dp_me, dp_me ^ 1, dp_me ^ 2, dp_me ^ 3]).astype(jnp.int32)
        d_inner = gate_w.shape[1] * fsdp_size
        d_model = norm_w.shape[1] * fsdp_size
        d_piece = d_model // 4
        o_piece = d_inner // 4
        w_in_t = jnp.transpose(w_in, (0, 2, 1))

        small_pieces = (norm_w, conv_w, conv_b, dt_bias, a_log, d_skip, gate_w)
        sizes = [p.size for p in small_pieces]
        order_q = [dp_me ^ bit for bit in range(4)]

        def slots(j):
            return [jnp.stack([me ^ j, q]) for q in order_q]
        natural = [jnp.stack([me ^ j, jnp.int32(q)]) for j in range(2) for q in range(4)]
        where = jnp.stack(natural + slots(2) + slots(3)).astype(jnp.int32)
        where_whole = [jnp.stack([order_f, jnp.zeros_like(order_f)], axis=1)] * 2

        def quarters_of(base, rows):
            q_rows = rows // 4
            return [lax.dynamic_slice(w_in_t, (0, base + (dp_me ^ bit) * q_rows, 0), (1, q_rows, d_piece))[0] for bit in (0, 3)]

        def far_of(p):
            return xor_perm(p, 'fsdp', 2)

        def far_spread(pair):
            return [pair[0], xor_perm(pair[0], 'dp', 1), xor_perm(pair[0], 'dp', 2), pair[1]]

        def join(p, near, far, axis):
            diag = [xor_perm(f, 'fsdp', 1) for f in far]
            if len(far) == 1:
                return assemble([p, near] + far + diag, where_whole[axis], axis, p.shape[0])
            return assemble([p, near] + far + diag, where, axis, p.shape[0] // 4)

        def near_of(p):
            return xor_perm(p, 'fsdp', 1)

        k_x = w_in_t.shape[1] - d_inner
        q_x0 = quarters_of(d_inner, k_x)
        far_x0 = [far_of(q) for q in q_x0]
        q_z0 = tie(*quarters_of(0, d_inner), *q_x0)[:2]
        far_z0 = [far_of(q) for q in q_z0]
        held = tie(*small_pieces, w_in_t, *q_z0)
        small_in, w_rest = held[:len(small_pieces)], held[len(small_pieces)]
        p_x0, p_z0 = w_rest[0, d_inner:], w_rest[0, :d_inner]
        near_x0, near_z0 = near_of(p_x0), near_of(p_z0)
        flat = jnp.concatenate([p.astype(F32).reshape(-1) for p in small_in])
        flat_rel = [flat] + [xor_perm(flat, 'fsdp', bit) for bit in (1, 2, 3)]
        all_x0 = far_spread(far_x0)
        all_z0 = far_spread(far_z0)

        flat_all = jnp.take(jnp.stack(flat_rel), order_f, axis=0)
        smalls = []
        lo = 0
        for p, size in zip(small_pieces, sizes):
            part = flat_all[:, lo:lo + size].reshape((fsdp_size,) + p.shape)
            smalls.append(jnp.moveaxis(part, 0, -2).reshape(p.shape[:-1] + (fsdp_size * p.shape[-1],)))
            lo += size
        norm_f, conv_f, convb_f, dtb_f, alog_f, dskip_f, gate_f = smalls
        cw_k = [conv_params(conv_f[n], convb_f[n]) for n in range(2)]
        hv_k = [head_params(dtb_f[n], alog_f[n], dskip_f[n]) for n in range(2)]
        gw_k = [gate_f[n][:, None] for n in range(2)]

        def proj(h, w_t):
            return dot_f32(w_t, h, ((1,), (0,))).astype(BF16)

        def out_proj(u_rows, n_t, w_o):
            return (u_rows.astype(F32) + dot_f32(w_o, n_t, ((0,), (0,)))).astype(BF16)

        h0 = pre_norm(u_in, norm_f[0])
        w_rest, o_rest, _ = tie(w_rest, w_out, *all_z0[:1])
        p_o0, p_x1, p_z1, p_o1 = o_rest[0], w_rest[1, d_inner:], w_rest[1, :d_inner], o_rest[1]
        far_o0, far_x1, far_z1, far_o1 = [[far_of(p)] for p in (p_o0, p_x1, p_z1, p_o1)]
        near_o0, near_x1, near_z1, near_o1 = [near_of(p) for p in (p_o0, p_x1, p_z1, p_o1)]
        wx0 = join(p_x0, near_x0, all_x0, 1)
        px0 = proj(h0, wx0)
        wz0 = join(p_z0, near_z0, all_z0, 1)
        pz0 = proj(h0, wz0)
        f0 = list(ssd_fwd(pz0, px0, cw_k[0], gw_k[0], hv_k[0]))
        f0[0], far_o0[0], far_x1[0] = tie(f0[0], far_o0[0], far_x1[0])
        wo0 = join(p_o0, near_o0, far_o0, 0)
        wx1 = join(p_x1, near_x1, far_x1, 1)
        hidden = out_proj(u_in, f0[0], wo0)
        h1 = pre_norm(hidden, norm_f[1])
        px1 = proj(h1, wx1)
        far_z1[0], px1 = tie(far_z1[0], px1)
        wz1 = join(p_z1, near_z1, far_z1, 1)
        pz1 = proj(h1, wz1)
        f1 = list(ssd_fwd(pz1, px1, cw_k[1], gw_k[1], hv_k[1]))
        f1[0], far_o1[0] = tie(f1[0], far_o1[0])
        wo1 = join(p_o1, near_o1, far_o1, 0)

        saved = ((u_in, h0, px0, pz0) + tuple(f0), (hidden, h1, px1, pz1) + tuple(f1))
        big = ((wx0, wz0, wo0), (wx1, wz1, wo1))

        def reduction(make, rows):
            sent = (make(1 - x_pos, 1 - core), make(x_pos, 1 - core))
            recv = yield sent, [xor_perm(s, 'fsdp', 1) for s in sent]
            away = make(1 - x_pos, core) + recv[0]
            far_in = xor_perm(away, 'fsdp', 2)
            part = make(x_pos, core) + recv[1]
            recv = yield (away, part), [far_in]
            piece = part + recv[0]
            quarters = piece.reshape(4, rows // 4, piece.shape[1])
            sent = [lax.dynamic_index_in_dim(quarters, dp_me ^ bit, 0, False) for bit in (3, 1, 2)]
            own = lax.dynamic_index_in_dim(quarters, dp_me, 0, False)
            recv = yield tuple(sent) + (own,), [xor_perm(s, 'dp', bit) for s, bit in zip(sent, (3, 1, 2))]
            total = own.astype(F32) + recv[0].astype(F32) + recv[1].astype(F32) + recv[2].astype(F32)
            got = yield (total,), [xor_perm(total, 'dp', bit) for bit in (3, 1, 2)]
            return [total, got[1], got[2], got[0]]

        def small_reduction(vec):
            for bit in (1, 2):
                recv = yield (vec,), [xor_perm(vec, 'fsdp', bit)]
                vec = vec + recv[0]
            recv = yield (vec,), [xor_perm(vec, 'dp', bit) for bit in (1, 2, 3)]
            return (vec + recv[0]) + (recv[1] + recv[2])

        live = []
        done = {}
        x_parts = ((('x0', 1184), ('x1', k_x - 1184)), (('x', k_x),))

        def launch(name, gen):
            sends, recvs = next(gen)
            live.append([name, gen, recvs])
            return list(sends)

        def advance(*anchors, only=None):
            picked = [item for item in live if not only or item[0] in only]
            if anchors:
                flat_in = [r for item in picked for r in item[2]]
                held = tie(*anchors, *flat_in)
                anchors, flat_in = list(held[:len(anchors)]), list(held[len(anchors):])
                for item in picked:
                    item[2] = [flat_in.pop(0) for _ in item[2]]
            sends = []
            for item in picked:
                try:
                    new_sends, item[2] = item[1].send(item[2])
                    sends.extend(new_sends)
                except StopIteration as stop:
                    done[item[0]] = stop.value
                    live.remove(item)
            return anchors, sends

        def backward(d_out, n, last, hold):
            u_rows, h, px, pz, n_t, y, st, cv, r, dt, cum, cumt = saved[n]
            w_x, w_z, w_o = big[n]

            def make_out(xp, c):
                rows = lax.dynamic_slice_in_dim(n_t, (2 * xp + c) * o_piece, o_piece, 0)
                return (dot_f32(rows, d_out, ((1,), (1,))) / batch_tot).astype(BF16)

            def make_in(d_t):
                def make(xp, c):
                    cols = lax.dynamic_slice_in_dim(h, (2 * xp + c) * d_piece, d_piece, 0)
                    return (dot_f32(d_t, cols, ((1,), (1,))) / batch_tot).astype(BF16)
                return make
            sends = launch(('o', n), reduction(make_out, o_piece))
            dn = proj(d_out, w_o)
            (dn,), more = advance(dn, only=[item[0] for item in live if item[0] not in hold])
            dn = tie(dn, *sends, *more)[0]
            dz, dy, gg = gate_bwd(pz, y, cv, dn, r, gw_k[n], hv_k[n])
            (dz, dy), more = advance(dz, dy)
            sends = launch(('z', n), reduction(make_in(dz), dz.shape[0]))
            d_h = dot_f32(w_z, dz, ((0,), (0,)))
            (d_h,), more2 = advance(d_h)
            dy = tie(dy, d_h, *sends, *more, *more2)[0]
            dpx, gcw, gh = ssd_bwd(px, cv, y, dy, st, dt, cum, cumt, cw_k[n], hv_k[n])
            (dpx,), more = advance(dpx)
            sends, lo, names = [], 0, []
            for part, rows in x_parts[n]:
                names.append((part, n))
                sends += launch(names[-1], reduction(make_in(dpx[lo:lo + rows]), rows))
                lo += rows
            dpx_h = tie(dpx, *sends, *more)[0]
            if last:
                more = advance(only=names)[1]
                dpx_h = tie(dpx_h, *more)[0]
            d_h = (d_h + dot_f32(w_x, dpx_h, ((0,), (0,)))).astype(BF16)
            d_norm, g_norm = pre_norm_bwd(u_rows, norm_f[n], d_h)
            d_u = (d_out.astype(F32) + d_norm.astype(F32)).astype(BF16)
            gh = jnp.sum(gh, axis=-1) / batch_tot
            half = lambda g: (g / batch_tot).astype(BF16).astype(F32)
            small = (half(g_norm), half(gcw[:, :4].T), half(gcw[:, 4]), gh[0], gh[1], gh[2], half(jnp.sum(gg, axis=-1)))
            if not last:
                (d_u,), more = advance(d_u, only=names)
                d_u = tie(d_u, *more)[0]
            return d_u, jnp.concatenate([s.reshape(-1) for s in small]), more, names

        d_out1 = tie(grad_out, f1[0])[0]
        d_hidden, small_two, _, names = backward(d_out1, 1, False, [])
        d_u, small_one, away, names = backward(d_hidden, 0, True, names)
        out = out_proj(hidden, f1[0], wo1)
        advance(*away, only=[item[0] for item in live if item[0] not in names])
        advance(only=names)
        totals = advance()[1]
        launch('s', small_reduction(tie(jnp.stack([small_one, small_two]), *totals)[0]))
        while live:
            advance()

        g_small = []
        lo = 0
        for p in small_pieces:
            size = p.size * fsdp_size // 2
            whole = done['s'][:, lo:lo + size].reshape(p.shape[:-1] + (fsdp_size * p.shape[-1],))
            g_small.append(lax.dynamic_slice_in_dim(whole, me * p.shape[-1], p.shape[-1], p.ndim - 1))
            lo += size

        def finish(parts, shape):
            blocks, plan = [], []
            for n in (1, 0):
                base = 0
                for part in parts[n]:
                    for j, blk in enumerate(done[(part, n)]):
                        blocks.append(blk)
                        plan.append((n, base, j))
                    base += 4 * blk.shape[0]
            return place(blocks, plan, order_d, shape)
        g_out = finish('oo', w_out.shape)
        g_in = jnp.transpose(finish([('z',) + tuple(p for p, _ in x_parts[n]) for n in range(2)], w_in_t.shape), (0, 2, 1))
        g_norm, g_conv, g_convb, g_dtb, g_alog, g_dskip, g_gate = g_small
        return out.T[None], d_u.T[None], g_norm, g_in, g_conv, g_convb, g_dtb, g_alog, g_dskip, g_gate, g_out

    return jax.shard_map(per_device, mesh=mesh, in_specs=(act_spec, act_spec) + weight_specs, out_specs=(act_spec, act_spec) + weight_specs, check_vma=False)
```

```python
import functools
import jax
import jax.numpy as jnp
from jax import lax
from jax.sharding import PartitionSpec as P
from jax.experimental import pallas as pl
from jax.experimental.pallas import tpu as pltpu

F32 = jnp.float32
BF16 = jnp.bfloat16
NORM_EPS = 1e-5
LOG2E = 1.4426950408889634
Q = 128
HP = 64
NS = 128
NN = (((1,), (0,)), ((), ()))
NT = (((1,), (1,)), ((), ()))
TN = (((0,), (0,)), ((), ()))


def mm(a, b, dims=NN):
    return lax.dot_general(a, b, dims, preferred_element_type=F32)


def sigm(v):
    return 0.5 * jnp.tanh(0.5 * v) + 0.5


def blocks_of(total, size):
    return [(lo, min(size, total - lo)) for lo in range(0, total, size)]


def row_loop(total, size):
    def run(body):
        @pl.loop(0, total // size)
        def _(i):
            body(pl.ds(pl.multiple_of(i * size, size), size))
    return run


def whole(arr_shape):
    zeros = (0,) * len(arr_shape)
    return pl.BlockSpec(arr_shape, lambda c: zeros)


def by_token(rows, n_rev=None):
    return pl.BlockSpec((rows, Q), lambda c: (0, c if n_rev is None else n_rev - c))


def by_chunk(rows, n_rev=None):
    return pl.BlockSpec((None, rows, Q), lambda c: (c if n_rev is None else n_rev - c, 0, 0))


def params(vmem=56 << 20):
    return pltpu.CompilerParams(dimension_semantics=("arbitrary",), vmem_limit_bytes=vmem)


def cost(flops):
    return pl.CostEstimate(flops=flops, bytes_accessed=40_000_000, transcendentals=0)


SCAN = tuple(2 ** e for e in range(7))


def dt_kernel(pdt_ref, hv_ref, dt_ref, cum_ref, cumt_ref):
    n_heads, seq = dt_ref.shape
    lane = lane_iota(n_heads)
    cols = [slice(lo, lo + Q) for lo in range(0, seq, Q)]
    accs = []
    for cc in cols:
        raw = pdt_ref[:, cc].astype(F32) + hv_ref[0]
        dt = jnp.maximum(raw, 0.0) + jnp.log1p(jnp.exp(-jnp.abs(raw)))
        dt_ref[:, cc] = dt
        accs.append(dt * hv_ref[1])
    for k in SCAN:
        accs = [acc + jnp.where(lane >= k, pltpu.roll(acc, k, 1), 0.0) for acc in accs]
    for cc, acc in zip(cols, accs):
        cum_ref[:, cc] = acc
        cumt_ref[cc, :] = jnp.transpose(acc)


def lane_iota(rows):
    return lax.broadcasted_iota(jnp.int32, (rows, Q), 1)


EXPC, EXPE, EXPT, CUM2, DT, SKIP, N_ROWS = range(7)
TAPS = 4
GRP = 4
PER = 4
RB = 256


def causal_mask():
    return lax.broadcasted_iota(jnp.int32, (Q, Q), 0) <= lax.broadcasted_iota(jnp.int32, (Q, Q), 1)


def fill_rows(rows_s, cum, dt, skip):
    tot = jnp.broadcast_to(cum[:, Q - 1:Q], cum.shape)
    for a, v in ((EXPC, jnp.exp(cum)), (EXPE, jnp.exp(tot - cum)), (EXPT, jnp.exp(tot)), (CUM2, cum * LOG2E), (DT, dt), (SKIP, skip)):
        rows_s[a] = v


def fold8(v):
    parts = [v[lo:lo + 8, :] for lo in range(0, v.shape[0], 8)]
    while len(parts) > 1:
        parts = [a + b for a, b in zip(parts[::2], parts[1::2])]
    return parts[0]


def ssd_fwd_kernel(n_heads, pz_ref, px_ref, cw_ref, gw_ref, hv_ref, dt_ref, cum_ref, cumt_ref,
                   n_ref, y_ref, s_ref, cv_ref, r_ref,
                   wb, gb, xprev, xs, vs, gt_s, st, rows_s):
    step = pl.program_id(0)
    d_inner = n_heads * HP
    conv_dim = d_inner + 2 * NS

    @pl.when(step == 0)
    def _():
        @row_loop(conv_dim, RB)
        def _(rr):
            for k in range(TAPS + 1):
                wb[k, rr, :] = jnp.broadcast_to(cw_ref[rr, k:k + 1], (RB, Q))
            xprev[rr, :] = jnp.zeros((RB, Q), BF16)

        @row_loop(d_inner, RB)
        def _(rr):
            gb[rr, :] = jnp.broadcast_to(gw_ref[rr, 0:1], (RB, Q))
            st[rr, :] = jnp.zeros((RB, NS), F32)

    @row_loop(conv_dim, RB)
    def _(rr):
        lane = lane_iota(RB)
        raw = px_ref[rr, :]
        x = raw.astype(F32)
        xp = xprev[rr, :].astype(F32)
        xprev[rr, :] = raw
        shifted = [pltpu.roll(jnp.where(lane >= Q - j, xp, x), j, 1) for j in range(1, TAPS)]
        acc = wb[TAPS, rr, :] + wb[TAPS - 1, rr, :] * x
        for j in range(1, TAPS):
            acc = acc + wb[TAPS - 1 - j, rr, :] * shifted[j - 1]
        cv_ref[rr, :] = acc
        xs[rr, :] = acc * sigm(acc)

    bt = xs[d_inner:d_inner + NS, :].astype(BF16)
    ct = xs[d_inner + NS:, :].astype(BF16)
    gt_s[...] = jnp.where(causal_mask(), mm(bt, ct, TN), 0.0)
    fill_rows(rows_s, cum_ref[...], dt_ref[...], hv_ref[2])
    cumt = cumt_ref[...] * LOG2E

    ssq = jnp.zeros((8, Q), F32)
    for lo in range(0, n_heads, GRP):
        gg = slice(lo * HP, (lo + GRP) * HP)
        st_g = st[gg, :]
        s_ref[gg, :] = st_g
        yoff = mm(st_g.astype(BF16), ct)
        xe = []
        for k in range(GRP):
            h = lo + k
            row = lambda a: rows_s[a, h:h + 1, :]
            hh = slice(h * HP, (h + 1) * HP)
            x = xs[hh, :]
            xdt = x * row(DT)
            gap = row(CUM2) - cumt[:, h:h + 1]
            mt = (gt_s[...] * jnp.exp2(jnp.minimum(gap, 0.0))).astype(BF16)
            y = mm(xdt.astype(BF16), mt) + yoff[k * HP:(k + 1) * HP, :] * row(EXPC)
            y_ref[hh, :] = y
            z = pz_ref[hh, :].astype(F32)
            v = (y + row(SKIP) * x) * (z * sigm(z))
            vs[hh, :] = v
            ssq = ssq + fold8(v * v)
            xe.append((xdt * row(EXPE)).astype(BF16))
        upd = mm(jnp.concatenate(xe, axis=0), bt, NT)
        for k in range(GRP):
            h = lo + k
            hh = slice(h * HP, (h + 1) * HP)
            st[hh, :] = st[hh, :] * rows_s[EXPT, h:h + 1, :] + upd[k * HP:(k + 1) * HP, :]

    r = lax.rsqrt(jnp.sum(ssq, axis=0, keepdims=True) / d_inner + NORM_EPS)
    r_ref[:, :] = r

    @row_loop(d_inner, RB)
    def _(rr):
        n_ref[rr, :] = (vs[rr, :] * r * gb[rr, :]).astype(BF16)


def head_params(dt_bias, a_log, d_skip):
    return jnp.broadcast_to(jnp.stack([dt_bias, -jnp.exp(a_log), d_skip])[:, :, None], (3, dt_bias.shape[0], Q))


def conv_params(conv_w, conv_b):
    return jnp.concatenate([conv_w.astype(F32), conv_b.astype(F32)[None]], axis=0).T


def ssd_dt(px, hv):
    n_heads = hv.shape[1]
    seq = px.shape[1]
    last = px.shape[0] // n_heads - 1
    shapes = [(n_heads, seq), (n_heads, seq), (seq, n_heads)]
    return pl.pallas_call(
        dt_kernel, grid=(1,),
        in_specs=[pl.BlockSpec((n_heads, seq), lambda c: (last, c)), whole(hv.shape)],
        out_specs=[whole(s) for s in shapes], out_shape=[jax.ShapeDtypeStruct(s, F32) for s in shapes],
        compiler_params=params(16 << 20), name="ssd_dt",
    )(px, hv)


def ssd_fwd(pz, px, cw, gw, hv):
    d_inner, seq = pz.shape
    conv_dim = cw.shape[0]
    n_heads = hv.shape[1]
    n_chunk = seq // Q
    dt, cum, cumt = ssd_dt(px, hv)
    f32s = lambda *s: jax.ShapeDtypeStruct(s, F32)
    outs = pl.pallas_call(
        functools.partial(ssd_fwd_kernel, n_heads),
        grid=(n_chunk,),
        in_specs=[by_token(d_inner), by_token(px.shape[0]), whole(cw.shape), whole(gw.shape), whole(hv.shape),
                  by_token(n_heads), by_token(n_heads), pl.BlockSpec((Q, n_heads), lambda c: (c, 0))],
        out_specs=[by_token(d_inner), by_chunk(d_inner), by_chunk(d_inner), by_chunk(conv_dim), by_token(1)],
        out_shape=[jax.ShapeDtypeStruct((d_inner, seq), BF16), f32s(n_chunk, d_inner, Q), f32s(n_chunk, d_inner, NS), f32s(n_chunk, conv_dim, Q), f32s(1, seq)],
        scratch_shapes=[pltpu.VMEM((TAPS + 1, conv_dim, Q), F32), pltpu.VMEM((d_inner, Q), F32), pltpu.VMEM((conv_dim, Q), BF16),
                        pltpu.VMEM((conv_dim, Q), F32), pltpu.VMEM((d_inner, Q), F32), pltpu.VMEM((Q, Q), F32),
                        pltpu.VMEM((d_inner, NS), F32), pltpu.VMEM((N_ROWS, n_heads, Q), F32)],
        compiler_params=params(), cost_estimate=cost(30_000_000_000), name="ssd_fwd",
    )(pz, px, cw, gw, hv, dt, cum, cumt)
    return tuple(outs) + (dt, cum, cumt)


def gate_bwd_kernel(n_heads, pz_ref, y_ref, cv_ref, dn_ref, r_ref, gw_ref, hv_ref,
                    dz_ref, dy_ref, gg_ref, gb, sk):
    step = pl.program_id(0)
    d_inner = n_heads * HP

    @pl.when(step == 0)
    def _():
        @row_loop(d_inner, RB)
        def _(rr):
            gb[rr, :] = jnp.broadcast_to(gw_ref[rr, 0:1], (RB, Q))
            gg_ref[rr, :] = jnp.zeros((RB, Q), F32)
        sk[...] = hv_ref[2]
    r = r_ref[:, :]
    per = PER

    def rows(i):
        return pl.ds(pl.multiple_of(i * (per * HP), per * HP), per * HP)

    def pass1(i, acc):
        rr = rows(i)
        cv = cv_ref[rr, :]
        x = cv * sigm(cv)
        skip = jnp.concatenate([jnp.broadcast_to(sk[pl.ds(i * per + k, 1), :], (HP, Q)) for k in range(per)], axis=0)
        yf = y_ref[rr, :] + skip * x
        dy_ref[rr, :] = yf
        z = pz_ref[rr, :].astype(F32)
        t = dn_ref[rr, :].astype(F32) * (yf * (z * sigm(z)) * r)
        gg_ref[rr, :] = gg_ref[rr, :] + t
        return acc + fold8(t * gb[rr, :])
    acc = lax.fori_loop(0, n_heads // per, pass1, jnp.zeros((8, Q), F32))
    mean = jnp.sum(acc, axis=0, keepdims=True) / d_inner

    @pl.loop(0, n_heads // per)
    def _(i):
        rr = rows(i)
        z = pz_ref[rr, :].astype(F32)
        yf = dy_ref[rr, :]
        sg = sigm(z)
        sl = z * sg
        dv = r * (dn_ref[rr, :].astype(F32) * gb[rr, :] - (yf * sl * r) * mean)
        dy_ref[rr, :] = dv * sl
        dz_ref[rr, :] = (dv * yf * (sg + sl * (1.0 - sg))).astype(BF16)


def gate_bwd(pz, y, cv, dn, r, gw, hv):
    d_inner, seq = pz.shape
    n_heads = hv.shape[1]
    return pl.pallas_call(
        functools.partial(gate_bwd_kernel, n_heads),
        grid=(seq // Q,),
        in_specs=[by_token(d_inner), by_chunk(d_inner), by_chunk(d_inner), by_token(d_inner), by_token(1), whole(gw.shape), whole(hv.shape)],
        out_specs=[by_token(d_inner), by_chunk(d_inner), whole((d_inner, Q))],
        out_shape=[jax.ShapeDtypeStruct((d_inner, seq), BF16), jax.ShapeDtypeStruct(y.shape, F32),
                   jax.ShapeDtypeStruct((d_inner, Q), F32)],
        scratch_shapes=[pltpu.VMEM((d_inner, Q), F32), pltpu.VMEM((n_heads, Q), F32)],
        compiler_params=params(), cost_estimate=cost(15_000_000_000), name="gate_bwd",
    )(pz, y, cv, dn, r, gw, hv)


def ssd_bwd_kernel(n_heads, n_chunk, px_ref, cv_ref, y_ref, dy_ref, s_ref, dt_ref, cum_ref, cumt_ref, cw_ref, hv_ref,
                   dpx_ref, gcw_ref, gh_ref,
                   wb, acc_w, dbuf, ds, gt_s, dg_s, rows_s, red_s, dbc):
    step = pl.program_id(0)
    d_inner = n_heads * HP
    conv_dim = d_inner + 2 * NS

    @pl.when(step == 0)
    def _():
        @row_loop(conv_dim, RB)
        def _(rr):
            for k in range(TAPS + 1):
                wb[k, rr, :] = jnp.broadcast_to(cw_ref[rr, k:k + 1], (RB, Q))
                acc_w[k, rr, :] = jnp.zeros((RB, Q), F32)
            dbuf[1, rr, :] = jnp.zeros((RB, Q), F32)

        @row_loop(d_inner, RB)
        def _(rr):
            ds[rr, :] = jnp.zeros((RB, NS), F32)
        gh_ref[...] = jnp.zeros(gh_ref.shape, F32)
    now = lax.rem(step, 2)
    later = 1 - now

    def act(cv):
        sg = sigm(cv)
        a = cv * sg
        return a, sg + a * (1.0 - sg)

    br = slice(d_inner, d_inner + NS)
    cr = slice(d_inner + NS, conv_dim)
    b_act, b_der = act(cv_ref[br, :])
    c_act, c_der = act(cv_ref[cr, :])
    bt = b_act.astype(BF16)
    ct = c_act.astype(BF16)
    gt_s[...] = jnp.where(causal_mask(), mm(bt, ct, TN), 0.0)
    fill_rows(rows_s, cum_ref[...], dt_ref[...], hv_ref[2])
    cumt = cumt_ref[...] * LOG2E
    d_a_sum, d_cum, d_dt = range(3)

    for lo in range(0, n_heads, GRP):
        gg = slice(lo * HP, (lo + GRP) * HP)
        ds_b = ds[gg, :].astype(BF16)
        sp_b = s_ref[gg, :].astype(BF16)
        dsb = mm(ds_b, bt)
        dye, xde, dgs = [], [], []
        for k in range(GRP):
            h = lo + k
            hh = slice(h * HP, (h + 1) * HP)
            kk = slice(k * HP, (k + 1) * HP)
            row = lambda a: rows_s[a, h:h + 1, :]
            total = lambda v: jnp.sum(v, axis=0, keepdims=True)
            x, der = act(cv_ref[hh, :])
            xdt = x * row(DT)
            xdt_b = xdt.astype(BF16)
            dy = dy_ref[hh, :]
            dy_b = dy.astype(BF16)
            dmt = mm(xdt_b, dy_b, TN)
            dec = jnp.exp2(jnp.minimum(row(CUM2) - cumt[:, h:h + 1], 0.0))
            mt = (gt_s[...] * dec).astype(BF16)
            dgs.append(dmt * dec)
            t2 = dsb[kk, :] * row(EXPE)
            dxdt = mm(dy_b, mt, NT) + t2
            xdt_r = xdt_b.astype(F32)
            red_s[d_dt, h:h + 1, :] = total(dxdt * x)
            red_s[d_cum, h:h + 1, :] = total(dy_b.astype(F32) * y_ref[hh, :] - xdt_r * dxdt)
            red_s[d_a_sum, h:h + 1, :] = total(xdt_r * t2 + row(EXPT) * (ds[hh, :] * s_ref[hh, :]))
            gh_ref[2, h:h + 1, :] = gh_ref[2, h:h + 1, :] + total(dy * x)
            dye.append((dy * row(EXPC)).astype(BF16))
            xde.append((xdt * row(EXPE)).astype(BF16))
            dbuf[now, hh, :] = (dxdt * row(DT) + row(SKIP) * dy) * der
        dye = jnp.concatenate(dye, axis=0)
        xde = jnp.concatenate(xde, axis=0)
        dg = (dgs[0] + dgs[1]) + (dgs[2] + dgs[3])
        d_b, d_c = mm(ds_b, xde, TN), mm(sp_b, dye, TN)
        if lo == 0:
            dg_s[...], dbc[0], dbc[1] = dg, d_b, d_c
        else:
            dg_s[...] = dg_s[...] + dg
            dbc[0] = dbc[0] + d_b
            dbc[1] = dbc[1] + d_c
        upd = mm(dye, ct, NT)
        for k in range(GRP):
            h = lo + k
            hh = slice(h * HP, (h + 1) * HP)
            ds[hh, :] = ds[hh, :] * rows_s[EXPT, h:h + 1, :] + upd[k * HP:(k + 1) * HP, :]

    dg = jnp.where(causal_mask(), dg_s[...], 0.0).astype(BF16)
    dbuf[now, br, :] = (dbc[0] + mm(ct, dg, NT)) * b_der
    dbuf[now, cr, :] = (dbc[1] + mm(bt, dg)) * c_der

    lane = lane_iota(n_heads)
    suf = red_s[d_cum]
    for k in SCAN:
        suf = suf + jnp.where(lane < Q - k, pltpu.roll(suf, Q - k, 1), 0.0)
    d_a = suf + jnp.broadcast_to(jnp.sum(red_s[d_a_sum], axis=1, keepdims=True), (n_heads, Q))
    raw_dt = px_ref[conv_dim:, :].astype(F32) + hv_ref[0]
    d_raw = (red_s[d_dt] + d_a * hv_ref[1]) * sigm(raw_dt)
    dpx_ref[conv_dim:, :] = d_raw.astype(BF16)
    gh_ref[0] = gh_ref[0] + d_raw
    gh_ref[1] = gh_ref[1] + d_a * dt_ref[...] * hv_ref[1]

    @row_loop(conv_dim, RB)
    def _(rr):
        lane = lane_iota(RB)
        raw = px_ref[rr, :].astype(F32)
        nxt = dbuf[later, rr, :]
        dcv = dbuf[now, rr, :]
        shifted = [pltpu.roll(jnp.where(lane < j, nxt, dcv), Q - j, 1) for j in range(1, TAPS)]
        acc_w[TAPS, rr, :] = acc_w[TAPS, rr, :] + dcv
        dx = 0.0
        for j, sh in enumerate([dcv] + shifted):
            tap = TAPS - 1 - j
            acc_w[tap, rr, :] = acc_w[tap, rr, :] + sh * raw
            dx = dx + wb[tap, rr, :] * sh
        dpx_ref[rr, :] = dx.astype(BF16)

    @pl.when(step == n_chunk - 1)
    def _():
        @row_loop(conv_dim, RB)
        def _(rr):
            lane = lane_iota(RB)
            out = jnp.zeros((RB, Q), F32)
            for k in range(TAPS + 1):
                out = jnp.where(lane == k, jnp.sum(acc_w[k, rr, :], axis=1, keepdims=True), out)
            gcw_ref[rr, :] = out


def ssd_bwd(px, cv, y, dy, states, dt, cum, cumt, cw, hv):
    n_chunk, d_inner, _ = y.shape
    conv_dim, seq = cw.shape[0], px.shape[1]
    n_heads = hv.shape[1]
    rev = n_chunk - 1
    rows = px.shape[0]
    tok = lambda n: by_token(n, rev)
    chunk = lambda n: by_chunk(n, rev)
    taps = pltpu.VMEM((TAPS + 1, conv_dim, Q), F32)
    square = pltpu.VMEM((Q, Q), F32)
    return pl.pallas_call(
        functools.partial(ssd_bwd_kernel, n_heads, n_chunk),
        grid=(n_chunk,),
        in_specs=[tok(rows), chunk(conv_dim), chunk(d_inner), chunk(d_inner), chunk(d_inner),
                  tok(n_heads), tok(n_heads), pl.BlockSpec((Q, n_heads), lambda c: (rev - c, 0)),
                  whole(cw.shape), whole(hv.shape)],
        out_specs=[tok(rows), whole((conv_dim, Q)), whole(hv.shape)],
        out_shape=[jax.ShapeDtypeStruct((rows, seq), BF16), jax.ShapeDtypeStruct((conv_dim, Q), F32),
                   jax.ShapeDtypeStruct(hv.shape, F32)],
        scratch_shapes=[taps, taps, pltpu.VMEM((2, conv_dim, Q), F32), pltpu.VMEM((d_inner, NS), F32), square, square,
                        pltpu.VMEM((N_ROWS, n_heads, Q), F32), pltpu.VMEM((3, n_heads, Q), F32), pltpu.VMEM((2, NS, Q), F32)],
        compiler_params=params(), cost_estimate=cost(60_000_000_000), name="ssd_bwd",
    )(px, cv, y, dy, states, dt, cum, cumt, cw, hv)


def xor_perm(x, axis, bit, size=4):
    return lax.ppermute(x, axis, [(i, i ^ bit) for i in range(size)])


def tie(*xs):
    return lax.optimization_barrier(xs)


def assemble_kernel(starts, n_src, order_ref, *refs):
    k = pl.program_id(0)
    ends = starts[1:] + (pl.num_programs(0),)
    for j in range(n_src):
        @pl.when((k >= starts[j]) & (k < ends[j]))
        def _(j=j):
            refs[n_src][...] = refs[j][...]


def assemble(sources, where, axis, rb):
    cols = sources[0].shape[1]
    counts = [src.shape[0] // rb for src in sources]
    starts = tuple(sum(counts[:j]) for j in range(len(counts)))
    n_steps = sum(counts)
    per = n_steps // 4

    def in_spec(j):
        return pl.BlockSpec((rb, cols), lambda k, o: (jnp.clip(k - starts[j], 0, counts[j] - 1), 0))
    if axis:
        shape, out_map = (per * rb, 4 * cols), lambda k, o: (o[k, 1], o[k, 0])
    else:
        shape, out_map = (n_steps * rb, cols), lambda k, o: (o[k, 0] * per + o[k, 1], 0)
    return pl.pallas_call(
        functools.partial(assemble_kernel, starts, len(sources)),
        grid_spec=pltpu.PrefetchScalarGridSpec(
            num_scalar_prefetch=1, grid=(n_steps,), in_specs=[in_spec(j) for j in range(len(sources))],
            out_specs=pl.BlockSpec((rb, cols), out_map)),
        out_shape=jax.ShapeDtypeStruct(shape, sources[0].dtype),
        compiler_params=params(40 << 20), cost_estimate=cost(3_000_000_000), name="assemble",
    )(where, *sources)


def place_kernel(plan, n_in, order_ref, *refs):
    out_ref, sem = refs[n_in], refs[n_in + 1]
    copies = []
    for k, (layer, base, j) in enumerate(plan):
        rows = refs[k].shape[0]
        lo = pl.multiple_of(base + order_ref[j] * rows, 8)
        copies.append(pltpu.make_async_copy(refs[k], out_ref.at[layer, pl.ds(lo, rows), :], sem.at[k]))
    for c in copies:
        c.start()
    for c in copies:
        c.wait()


def place(blocks, plan, order, shape):
    n_in = len(blocks)
    return pl.pallas_call(
        functools.partial(place_kernel, plan, n_in),
        in_specs=[pl.BlockSpec(memory_space=pltpu.SMEM)] + [pl.BlockSpec(memory_space=pltpu.VMEM)] * n_in,
        out_specs=pl.BlockSpec(memory_space=pl.ANY),
        out_shape=jax.ShapeDtypeStruct(shape, F32),
        scratch_shapes=[pltpu.SemaphoreType.DMA((n_in,))],
        compiler_params=pltpu.CompilerParams(vmem_limit_bytes=40 << 20),
        name="place",
    )(order, *blocks)


def dot_f32(a, b, dims):
    return lax.dot_general(a, b, (dims, ((), ())), preferred_element_type=F32)


def pre_norm(u_rows, norm_w):
    rows_f = u_rows.astype(F32)
    inv_rms = lax.rsqrt(jnp.mean(jnp.square(rows_f), axis=0, keepdims=True) + NORM_EPS)
    return (rows_f * inv_rms * norm_w[:, None]).astype(BF16)


def pre_norm_bwd(u_rows, norm_w, d_h):
    rows_f = u_rows.astype(F32)
    inv_rms = lax.rsqrt(jnp.mean(jnp.square(rows_f), axis=0, keepdims=True) + NORM_EPS)
    d_f = d_h.astype(F32)
    unit = rows_f * inv_rms
    g_w = jnp.sum(d_f * unit, axis=1)
    d_unit = d_f * norm_w[:, None]
    d_rows = inv_rms * (d_unit - unit * jnp.mean(d_unit * unit, axis=0, keepdims=True))
    return d_rows.astype(BF16), g_w


def solution(mesh):
    dp_size = mesh.shape['dp']
    fsdp_size = mesh.shape['fsdp']
    act_spec = P(('dp', 'fsdp'), None, None)
    weight_specs = (P(None, 'fsdp'), P(None, 'fsdp', None), P(None, None, 'fsdp'), P(None, 'fsdp'), P(None, 'fsdp'), P(None, 'fsdp'), P(None, 'fsdp'), P(None, 'fsdp'), P(None, 'fsdp', None))

    def per_device(u_loc, g_loc, norm_w, w_in, conv_w, conv_b, dt_bias, a_log, d_skip, gate_w, w_out):
        batch_tot = u_loc.shape[0] * dp_size * fsdp_size
        u_in, grad_out = u_loc[0].T, g_loc[0].T
        me = lax.axis_index('fsdp')
        dp_me = lax.axis_index('dp')
        core = me % 2
        x_pos = me // 2
        order_f = jnp.stack([me, me ^ 1, me ^ 2, me ^ 3]).astype(jnp.int32)
        order_d = jnp.stack([dp_me, dp_me ^ 1, dp_me ^ 2, dp_me ^ 3]).astype(jnp.int32)
        d_inner = gate_w.shape[1] * fsdp_size
        d_model = norm_w.shape[1] * fsdp_size
        d_piece = d_model // 4
        o_piece = d_inner // 4
        w_in_t = jnp.transpose(w_in, (0, 2, 1))

        small_pieces = (norm_w, conv_w, conv_b, dt_bias, a_log, d_skip, gate_w)
        sizes = [p.size for p in small_pieces]
        order_q = [dp_me ^ bit for bit in range(4)]

        def slots(j):
            return [jnp.stack([me ^ j, q]) for q in order_q]
        natural = [jnp.stack([me ^ j, jnp.int32(q)]) for j in range(2) for q in range(4)]
        where = jnp.stack(natural + slots(2) + slots(3)).astype(jnp.int32)
        where_whole = [jnp.stack([order_f, jnp.zeros_like(order_f)], axis=1)] * 2

        def quarters_of(base, rows):
            q_rows = rows // 4
            return [lax.dynamic_slice(w_in_t, (0, base + (dp_me ^ bit) * q_rows, 0), (1, q_rows, d_piece))[0] for bit in (0, 3)]

        def far_of(p):
            return xor_perm(p, 'fsdp', 2)

        def far_spread(pair):
            return [pair[0], xor_perm(pair[0], 'dp', 1), xor_perm(pair[0], 'dp', 2), pair[1]]

        def join(p, near, far, axis):
            diag = [xor_perm(f, 'fsdp', 1) for f in far]
            if len(far) == 1:
                return assemble([p, near] + far + diag, where_whole[axis], axis, p.shape[0])
            return assemble([p, near] + far + diag, where, axis, p.shape[0] // 4)

        def near_of(p):
            return xor_perm(p, 'fsdp', 1)

        k_x = w_in_t.shape[1] - d_inner
        q_x0 = quarters_of(d_inner, k_x)
        far_x0 = [far_of(q) for q in q_x0]
        q_z0 = tie(*quarters_of(0, d_inner), *q_x0)[:2]
        far_z0 = [far_of(q) for q in q_z0]
        held = tie(*small_pieces, w_in_t, *q_z0)
        small_in, w_rest = held[:len(small_pieces)], held[len(small_pieces)]
        p_x0, p_z0 = w_rest[0, d_inner:], w_rest[0, :d_inner]
        near_x0, near_z0 = near_of(p_x0), near_of(p_z0)
        flat = jnp.concatenate([p.astype(F32).reshape(-1) for p in small_in])
        flat_rel = [flat] + [xor_perm(flat, 'fsdp', bit) for bit in (1, 2, 3)]
        all_x0 = far_spread(far_x0)
        all_z0 = far_spread(far_z0)

        flat_all = jnp.take(jnp.stack(flat_rel), order_f, axis=0)
        smalls = []
        lo = 0
        for p, size in zip(small_pieces, sizes):
            part = flat_all[:, lo:lo + size].reshape((fsdp_size,) + p.shape)
            smalls.append(jnp.moveaxis(part, 0, -2).reshape(p.shape[:-1] + (fsdp_size * p.shape[-1],)))
            lo += size
        norm_f, conv_f, convb_f, dtb_f, alog_f, dskip_f, gate_f = smalls
        cw_k = [conv_params(conv_f[n], convb_f[n]) for n in range(2)]
        hv_k = [head_params(dtb_f[n], alog_f[n], dskip_f[n]) for n in range(2)]
        gw_k = [gate_f[n][:, None] for n in range(2)]

        def proj(h, w_t):
            return dot_f32(w_t, h, ((1,), (0,))).astype(BF16)

        def out_proj(u_rows, n_t, w_o):
            return (u_rows.astype(F32) + dot_f32(w_o, n_t, ((0,), (0,)))).astype(BF16)

        h0 = pre_norm(u_in, norm_f[0])
        w_rest, o_rest, _ = tie(w_rest, w_out, *all_z0[:1])
        p_o0, p_x1, p_z1, p_o1 = o_rest[0], w_rest[1, d_inner:], w_rest[1, :d_inner], o_rest[1]
        far_o0, far_x1, far_z1, far_o1 = [[far_of(p)] for p in (p_o0, p_x1, p_z1, p_o1)]
        near_o0, near_x1, near_z1, near_o1 = [near_of(p) for p in (p_o0, p_x1, p_z1, p_o1)]
        wx0 = join(p_x0, near_x0, all_x0, 1)
        px0 = proj(h0, wx0)
        wz0 = join(p_z0, near_z0, all_z0, 1)
        pz0 = proj(h0, wz0)
        f0 = list(ssd_fwd(pz0, px0, cw_k[0], gw_k[0], hv_k[0]))
        f0[0], far_o0[0], far_x1[0] = tie(f0[0], far_o0[0], far_x1[0])
        wo0 = join(p_o0, near_o0, far_o0, 0)
        wx1 = join(p_x1, near_x1, far_x1, 1)
        hidden = out_proj(u_in, f0[0], wo0)
        h1 = pre_norm(hidden, norm_f[1])
        px1 = proj(h1, wx1)
        far_z1[0], px1 = tie(far_z1[0], px1)
        wz1 = join(p_z1, near_z1, far_z1, 1)
        pz1 = proj(h1, wz1)
        f1 = list(ssd_fwd(pz1, px1, cw_k[1], gw_k[1], hv_k[1]))
        f1[0], far_o1[0] = tie(f1[0], far_o1[0])
        wo1 = join(p_o1, near_o1, far_o1, 0)

        saved = ((u_in, h0, px0, pz0) + tuple(f0), (hidden, h1, px1, pz1) + tuple(f1))
        big = ((wx0, wz0, wo0), (wx1, wz1, wo1))

        def reduction(make, rows):
            sent = (make(1 - x_pos, 1 - core), make(x_pos, 1 - core))
            recv = yield sent, [xor_perm(s, 'fsdp', 1) for s in sent]
            away = make(1 - x_pos, core) + recv[0]
            far_in = xor_perm(away, 'fsdp', 2)
            part = make(x_pos, core) + recv[1]
            recv = yield (away, part), [far_in]
            piece = part + recv[0]
            quarters = piece.reshape(4, rows // 4, piece.shape[1])
            sent = [lax.dynamic_index_in_dim(quarters, dp_me ^ bit, 0, False) for bit in (3, 1, 2)]
            own = lax.dynamic_index_in_dim(quarters, dp_me, 0, False)
            recv = yield tuple(sent) + (own,), [xor_perm(s, 'dp', bit) for s, bit in zip(sent, (3, 1, 2))]
            total = own.astype(F32) + recv[0].astype(F32) + recv[1].astype(F32) + recv[2].astype(F32)
            got = yield (total,), [xor_perm(total, 'dp', bit) for bit in (3, 1, 2)]
            return [total, got[1], got[2], got[0]]

        def small_reduction(vec):
            for bit in (1, 2):
                recv = yield (vec,), [xor_perm(vec, 'fsdp', bit)]
                vec = vec + recv[0]
            recv = yield (vec,), [xor_perm(vec, 'dp', bit) for bit in (1, 2, 3)]
            return (vec + recv[0]) + (recv[1] + recv[2])

        live = []
        done = {}
        x_parts = ((('x0', 1184), ('x1', k_x - 1184)), (('x', k_x),))

        def launch(name, gen):
            sends, recvs = next(gen)
            live.append([name, gen, recvs])
            return list(sends)

        def advance(*anchors, only=None):
            picked = [item for item in live if not only or item[0] in only]
            if anchors:
                flat_in = [r for item in picked for r in item[2]]
                held = tie(*anchors, *flat_in)
                anchors, flat_in = list(held[:len(anchors)]), list(held[len(anchors):])
                for item in picked:
                    item[2] = [flat_in.pop(0) for _ in item[2]]
            sends = []
            for item in picked:
                try:
                    new_sends, item[2] = item[1].send(item[2])
                    sends.extend(new_sends)
                except StopIteration as stop:
                    done[item[0]] = stop.value
                    live.remove(item)
            return anchors, sends

        def backward(d_out, n, last, hold):
            u_rows, h, px, pz, n_t, y, st, cv, r, dt, cum, cumt = saved[n]
            w_x, w_z, w_o = big[n]

            def make_out(xp, c):
                rows = lax.dynamic_slice_in_dim(n_t, (2 * xp + c) * o_piece, o_piece, 0)
                return (dot_f32(rows, d_out, ((1,), (1,))) / batch_tot).astype(BF16)

            def make_in(d_t):
                def make(xp, c):
                    cols = lax.dynamic_slice_in_dim(h, (2 * xp + c) * d_piece, d_piece, 0)
                    return (dot_f32(d_t, cols, ((1,), (1,))) / batch_tot).astype(BF16)
                return make
            sends = launch(('o', n), reduction(make_out, o_piece))
            dn = proj(d_out, w_o)
            (dn,), more = advance(dn, only=[item[0] for item in live if item[0] not in hold])
            dn = tie(dn, *sends, *more)[0]
            dz, dy, gg = gate_bwd(pz, y, cv, dn, r, gw_k[n], hv_k[n])
            late = [('o', n)] if last else []
            (dz, dy), more = advance(dz, dy, only=[item[0] for item in live if item[0] not in late])
            sends = launch(('z', n), reduction(make_in(dz), dz.shape[0]))
            d_h = dot_f32(w_z, dz, ((0,), (0,)))
            (d_h,), more2 = advance(d_h)
            dy = tie(dy, d_h, *sends, *more, *more2)[0]
            dpx, gcw, gh = ssd_bwd(px, cv, y, dy, st, dt, cum, cumt, cw_k[n], hv_k[n])
            (dpx,), more = advance(dpx)
            sends, lo, names = [], 0, []
            for part, rows in x_parts[n]:
                names.append((part, n))
                sends += launch(names[-1], reduction(make_in(dpx[lo:lo + rows]), rows))
                lo += rows
            dpx_h = tie(dpx, *sends, *more)[0]
            if last:
                more = advance(only=names)[1]
                dpx_h = tie(dpx_h, *more)[0]
            d_h = (d_h + dot_f32(w_x, dpx_h, ((0,), (0,)))).astype(BF16)
            d_norm, g_norm = pre_norm_bwd(u_rows, norm_f[n], d_h)
            d_u = (d_out.astype(F32) + d_norm.astype(F32)).astype(BF16)
            gh = jnp.sum(gh, axis=-1) / batch_tot
            half = lambda g: (g / batch_tot).astype(BF16).astype(F32)
            small = (half(g_norm), half(gcw[:, :4].T), half(gcw[:, 4]), gh[0], gh[1], gh[2], half(jnp.sum(gg, axis=-1)))
            if not last:
                (d_u,), more = advance(d_u, only=names)
                d_u = tie(d_u, *more)[0]
            return d_u, jnp.concatenate([s.reshape(-1) for s in small]), more, names

        d_out1 = tie(grad_out, f1[0])[0]
        d_hidden, small_two, _, names = backward(d_out1, 1, False, [])
        d_u, small_one, away, names = backward(d_hidden, 0, True, names)
        out = out_proj(hidden, f1[0], wo1)
        advance(*away, only=[item[0] for item in live if item[0] not in names])
        advance(only=names)
        totals = advance()[1]
        launch('s', small_reduction(tie(jnp.stack([small_one, small_two]), *totals)[0]))
        while live:
            advance()

        g_small = []
        lo = 0
        for p in small_pieces:
            size = p.size * fsdp_size // 2
            whole = done['s'][:, lo:lo + size].reshape(p.shape[:-1] + (fsdp_size * p.shape[-1],))
            g_small.append(lax.dynamic_slice_in_dim(whole, me * p.shape[-1], p.shape[-1], p.ndim - 1))
            lo += size

        def finish(parts, shape):
            blocks, plan = [], []
            for n in (1, 0):
                base = 0
                for part in parts[n]:
                    for j, blk in enumerate(done[(part, n)]):
                        blocks.append(blk)
                        plan.append((n, base, j))
                    base += 4 * blk.shape[0]
            return place(blocks, plan, order_d, shape)
        g_out = finish('oo', w_out.shape)
        g_in = jnp.transpose(finish([('z',) + tuple(p for p, _ in x_parts[n]) for n in range(2)], w_in_t.shape), (0, 2, 1))
        g_norm, g_conv, g_convb, g_dtb, g_alog, g_dskip, g_gate = g_small
        return out.T[None], d_u.T[None], g_norm, g_in, g_conv, g_convb, g_dtb, g_alog, g_dskip, g_gate, g_out

    return jax.shard_map(per_device, mesh=mesh, in_specs=(act_spec, act_spec) + weight_specs, out_specs=(act_spec, act_spec) + weight_specs, check_vma=False)
```
